32 devices in a mesh: coil: 8 (over z, x), frame: 4 (over y, core).
Axes of the slice: x: 2, y: 2, z: 4, core: 2. Of those that a mesh axis runs over, the one named last changes fastest.
Arguments:
- initial_image: float32 [256, 4, 2, 256], P('coil', 'frame'), may hold values from -3 to 3
- coil_maps: bfloat16 [8, 2, 256, 256], P('coil'), may hold values from -2 to 2
- samples: bfloat16 [8, 4, 18, 2, 256], P('coil', 'frame'), may hold values from -6 to 6
- blocks_used: int32 [4], P('frame'), may hold values from 1 to 18, 37 in all
- row_offset: int32 [4, 18], P('frame'), may hold values from 0 to 128
- col_offset: int32 [4, 18], P('frame'), may hold values from 0 to 128
- row_first: int32 [4, 18, 256], P('frame'), may hold values from 0 to 124
- col_first: int32 [4, 18, 256], P('frame'), may hold values from 0 to 124
- row_taps: bfloat16 [4, 18, 4, 256], P('frame'), may hold values from 0.099609375 to 0.59765625
- col_taps: bfloat16 [4, 18, 4, 256], P('frame'), may hold values from 0.099609375 to 0.59765625
Outputs:
- image: float32 [256, 4, 2, 256], P('coil', 'frame')
- misfit: float32 [2, 4], P(None, 'frame')
The draws below stay inside these ranges and needn't reach their ends.
Inputs may be any that keep to these rules, and one draw needn't show every extreme that they name: Blocks 0 to blocks_used minus one of the frame were acquired. `row_first`: the kernel's 4 rows lie inside the tile. `col_first`: the kernel's 4 columns lie inside the tile.
All inputs are finite; a program needn't handle non-finite values.
Results may differ from the reference program's by a relative error of at most 0.006.
Values may be sent and summed in bfloat16 or wider, within the bound.
A program may use at most 64 MiB of HBM per device.

```python
import math
import jax
import jax.numpy as jnp
import numpy as np
from jax import lax

N = 256
COILS = 8
FRAMES = 4
NB = 18
BS = 256
TT = 128
KW = 4
ITERS = 2


def touch_ends(drawn, own_key, least, largest):
    longest = drawn.shape.index(max(drawn.shape))
    spots = []
    for shift in (0, 1):
        where = [jax.random.randint(jax.random.fold_in(own_key, axis), (), 0, length) for axis, length in enumerate(drawn.shape)]
        where[longest] = (where[longest] + shift) % drawn.shape[longest]
        spots.append(tuple(where))
    return drawn.at[spots[0]].set(least).at[spots[1]].set(largest)


def spiked(array, rng, source, target, parts, factor):
    def block_of(axis_at):
        return (jnp.arange(array.shape[axis_at]) // (array.shape[axis_at] // parts)).reshape((-1,) + (1,) * (array.ndim - 1 - axis_at))

    first = jax.random.permutation(rng, parts)[block_of(target)]
    far = (block_of(target) + parts // 2) % parts
    return jnp.where((block_of(source) == first) | (block_of(source) == far), factor * array, array)


def level_of(stream_key, shape, cuts, low, top_value):
    def one(position, blocks):
        draws = jax.random.uniform(jax.random.fold_in(jax.random.fold_in(stream_key, 6), position), (blocks,), jnp.float32, low / len(cuts), top_value / len(cuts))
        return jnp.repeat(jnp.exp(draws), shape[position] // blocks).reshape((-1,) + (1,) * (len(shape) - position - 1))

    factor_of = one(*cuts[0])
    for cut in cuts[1:]:
        factor_of = factor_of * one(*cut)
    return factor_of


def length_profile(count, total, most, slope):
    portions = [(1 << 20) // math.isqrt(standing ** slope) + 1 for standing in range(2, count + 1)]
    rest, counts = total - most - (count - 1), [1] * (count - 1)
    while rest > 0:
        candidates = [i for i in range(count - 1) if counts[i] < most]
        mass, remaining = sum([portions[i] for i in candidates]), rest
        for i in candidates:
            addition = min(most - counts[i], max(1, remaining * portions[i] // mass), rest)
            counts[i] = counts[i] + addition
            rest = rest - addition
    return np.array([most] + counts)


def uneven_parts(stream_key, count, total, reach, lean):
    if count == 2:
        one = jax.random.randint(stream_key, (), max(1, total - reach), min(reach, total - 1) + 1)
        return jnp.stack([one, total - one])
    lengths = jnp.asarray(length_profile(count, total, reach, lean), jnp.int32)
    twos = (count - 1) // 2
    giver, sink = lengths[1:1 + 2 * twos:2], lengths[2:2 + 2 * twos:2]
    slack = jnp.minimum(giver - 1, reach - sink)
    passed = jax.random.randint(jax.random.fold_in(stream_key, 1), (twos,), 0, 1 << 20) % (slack + 1)
    lengths = lengths.at[1:1 + 2 * twos:2].set(giver - passed).at[2:2 + 2 * twos:2].set(sink + passed)
    return lengths[jax.random.permutation(jax.random.fold_in(stream_key, 2), count)]


def centred(rng, shape, width, most, shards=(), kind=jnp.bfloat16):
    gain = level_of(rng, shape, shards, -0.22, 0.18) if shards else 1.0
    drawn = jax.random.normal(rng, shape, jnp.float32) * width * gain
    return jnp.minimum(jnp.maximum(drawn, -most), most).astype(kind)


def bell_draw_with(stream_key, shape, deviation, most, shards, heavy, kind=jnp.bfloat16):
    entries = deviation * jax.random.normal(stream_key, shape, jnp.float32)
    if shards:
        entries = entries * level_of(stream_key, shape, shards, -0.22, 0.18)
    return jnp.clip(spiked(entries, jax.random.fold_in(stream_key, 3), *heavy), -most, most).astype(kind)


def setup_inputs(seed: int = 0) -> dict:
    key_list = jax.random.split(jax.random.key(seed), 11)
    return {
        "initial_image": centred(key_list[0], (N, FRAMES, 2, N), 0.5, 3.0, ((0, 8), (1, 4)), jnp.float32),
        "coil_maps": bell_draw_with(key_list[1], (COILS, 2, N, N), (2 * COILS) ** -0.5, 2.0, ((0, 8),), (0, 2, 8, 2.0)),
        "samples": centred(key_list[2], (COILS, FRAMES, NB, 2, BS), 1.0, 6.0, ((0, 8), (1, 4))),
        "blocks_used": uneven_parts(key_list[3], FRAMES, FRAMES * NB // 2 + 1, NB, 2).astype(jnp.int32),
        "row_offset": touch_ends(jax.random.randint(key_list[4], (FRAMES, NB), 0, N - TT + 1), jax.random.fold_in(key_list[4], 1), 0, N - TT).astype(jnp.int32),
        "col_offset": touch_ends(jax.random.randint(key_list[5], (FRAMES, NB), 0, N - TT + 1), jax.random.fold_in(key_list[5], 1), 0, N - TT).astype(jnp.int32),
        "row_first": touch_ends(jax.random.randint(key_list[6], (FRAMES, NB, BS), 0, TT - KW + 1), jax.random.fold_in(key_list[6], 1), 0, TT - KW).astype(jnp.int32),
        "col_first": touch_ends(jax.random.randint(key_list[7], (FRAMES, NB, BS), 0, TT - KW + 1), jax.random.fold_in(key_list[7], 1), 0, TT - KW).astype(jnp.int32),
        "row_taps": jnp.clip(0.099609375 + 0.49804688 * jax.random.uniform(key_list[8], (FRAMES, NB, KW, BS), jnp.float32) ** level_of(key_list[8], (FRAMES, NB, KW, BS), ((0, 4),), -0.2, 0.2), 0.099609375, 0.59765625).astype(jnp.bfloat16),
        "col_taps": jnp.clip(0.099609375 + 0.49804688 * jax.random.uniform(key_list[9], (FRAMES, NB, KW, BS), jnp.float32) ** level_of(key_list[9], (FRAMES, NB, KW, BS), ((0, 4),), -0.2, 0.2), 0.099609375, 0.59765625).astype(jnp.bfloat16),
    }


step_size = 2.0
tv_weight = 0.1
smooth_floor = 0.5
shrink_weight = 0.1

def rounded(values):
    return lax.optimization_barrier(values.astype(jnp.bfloat16))

def pair_tables(order):
    counter = jnp.arange(order, dtype=jnp.int32)
    phase = counter[:, None] * counter[None, :] % order
    angle = phase.astype(jnp.float32) * (2.0 * math.pi / order)
    cosine = (jnp.cos(angle) / math.sqrt(order)).astype(jnp.bfloat16)
    sine = (jnp.sin(angle) / math.sqrt(order)).astype(jnp.bfloat16)
    table_one = jnp.stack([jnp.stack([cosine, sine]), jnp.stack([-sine, cosine])])
    table_two = jnp.stack([jnp.stack([cosine, -sine]), jnp.stack([sine, cosine])])
    return (table_one, table_two)

def tap_matrix(first_idx, taps):
    positions = jnp.arange(TT, dtype=jnp.int32)
    matrix = jnp.zeros((first_idx.shape[0], TT), jnp.float32)
    for offset in range(KW):
        hits = positions[None, :] == first_idx[:, None] + offset
        matrix = matrix + jnp.where(hits, taps[offset].astype(jnp.float32)[:, None], 0.0)
    return matrix.astype(jnp.bfloat16)

def spoke_block(kspace, grid_sum, tile_row, tile_col, first_row, first_col, taps_row, taps_col, measured, active):
    rows_matrix = tap_matrix(first_row, taps_row)
    cols_matrix = tap_matrix(first_col, taps_col)
    anchor = jnp.zeros((), jnp.int32)
    corner = (anchor, tile_row.astype(jnp.int32), tile_col.astype(jnp.int32))
    grid_tile = lax.dynamic_slice(kspace, corner, (2, TT, TT))
    across = jnp.einsum('si,pij->psj', rows_matrix.astype(jnp.float32), grid_tile.astype(jnp.float32))
    cols_wide = cols_matrix.astype(jnp.float32)
    predicted = lax.optimization_barrier(jnp.sum(across * cols_wide[None], axis=2))
    resid = (predicted - measured.astype(jnp.float32)) * active
    misfit = jnp.sum(resid * resid)
    resid_low = rounded(resid)
    weighted = rounded(resid_low.astype(jnp.float32)[:, :, None] * cols_wide[None])
    spread = jnp.einsum('si,psj->pij', rows_matrix.astype(jnp.float32), weighted.astype(jnp.float32))
    updated = lax.dynamic_slice(grid_sum, corner, (2, TT, TT)) + spread
    return (lax.dynamic_update_slice(grid_sum, updated, corner), misfit)

def frame_grid(kspace, count, row_off, col_off, row_idx, col_idx, row_w, col_w, measured):

    def visit(running, inputs):
        grid_sum, misfit_sum = running
        block_id, tile_row, tile_col, first_row, first_col, taps_row, taps_col, block_data = inputs
        active = (block_id < count).astype(jnp.float32)
        grid_sum, misfit = spoke_block(kspace, grid_sum, tile_row, tile_col, first_row, first_col, taps_row, taps_col, block_data, active)
        return ((grid_sum, misfit_sum + misfit), None)
    initial = (jnp.zeros((2, N, N), jnp.float32), jnp.zeros((), jnp.float32))
    blocks = jnp.arange(NB, dtype=jnp.int32)
    (grid_sum, misfit_sum), unused = lax.scan(visit, initial, (blocks, row_off, col_off, row_idx, col_idx, row_w, col_w, measured))
    return (rounded(grid_sum), misfit_sum)

def coil_forward(image_low, maps, table_one, table_two):
    maps_wide = maps.astype(jnp.float32)
    image_wide = image_low.astype(jnp.float32)
    real_part = maps_wide[0][:, None, :] * image_wide[:, :, 0] - maps_wide[1][:, None, :] * image_wide[:, :, 1]
    imag_part = maps_wide[0][:, None, :] * image_wide[:, :, 1] + maps_wide[1][:, None, :] * image_wide[:, :, 0]
    coil_image = rounded(jnp.stack([real_part, imag_part], axis=2))
    half = rounded(jnp.einsum('qprk,kfpn->fqrn', table_one.astype(jnp.float32), coil_image.astype(jnp.float32)))
    return rounded(jnp.einsum('fprk,pqkn->fqrn', half.astype(jnp.float32), table_two.astype(jnp.float32)))

def coil_adjoint(grid_low, maps, table_one, table_two):
    back_half = rounded(jnp.einsum('qprk,fpkn->fqrn', table_two.astype(jnp.float32), grid_low.astype(jnp.float32)))
    coil_back = jnp.einsum('fprk,pqkn->rfqn', back_half.astype(jnp.float32), table_one.astype(jnp.float32))
    maps_wide = maps.astype(jnp.float32)
    real_part = maps_wide[0][:, None, :] * coil_back[:, :, 0] + maps_wide[1][:, None, :] * coil_back[:, :, 1]
    imag_part = maps_wide[0][:, None, :] * coil_back[:, :, 1] - maps_wide[1][:, None, :] * coil_back[:, :, 0]
    return jnp.stack([real_part, imag_part], axis=2)

def cine_gradient(padded):
    change = padded[:, 1:] - padded[:, :-1]
    length = jnp.sqrt(lax.optimization_barrier(jnp.sum(change * change, axis=2, keepdims=True)) + smooth_floor * smooth_floor)
    normed = change / length
    return normed[:, :-1] - normed[:, 1:]

def shrink(detail, limit):
    length = jnp.sqrt(lax.optimization_barrier(jnp.sum(detail * detail, axis=2, keepdims=True)))
    return detail * (jnp.maximum(length - limit, 0.0) / jnp.maximum(length, limit))

def wavelet_prox(field, limit):
    even_rows = field[0::2]
    odd_rows = field[1::2]
    top_left = even_rows[..., 0::2]
    top_right = even_rows[..., 1::2]
    low_left = odd_rows[..., 0::2]
    low_right = odd_rows[..., 1::2]
    approx = (top_left + top_right + low_left + low_right) * 0.5
    horiz = shrink((top_left - top_right + low_left - low_right) * 0.5, limit)
    vertical = shrink((top_left + top_right - low_left - low_right) * 0.5, limit)
    diagonal = shrink((top_left - top_right - low_left + low_right) * 0.5, limit)
    new_tl = (approx + horiz + vertical + diagonal) * 0.5
    new_tr = (approx - horiz + vertical - diagonal) * 0.5
    new_ll = (approx + horiz - vertical - diagonal) * 0.5
    new_lr = (approx - horiz - vertical + diagonal) * 0.5
    top_rows = jnp.stack([new_tl, new_tr], axis=-1).reshape(even_rows.shape)
    low_rows = jnp.stack([new_ll, new_lr], axis=-1).reshape(odd_rows.shape)
    return jnp.stack([top_rows, low_rows], axis=1).reshape(field.shape)

def reference(initial_image, coil_maps, samples, blocks_used, row_offset, col_offset, row_first, col_first, row_taps, col_taps):
    table_one, table_two = pair_tables(N)
    grid_frames = jax.vmap(frame_grid)

    def data_term(image_low):

        def per_coil(running, inputs):
            grad_sum, misfit_sum = running
            maps, measured = inputs
            kspace = coil_forward(image_low, maps, table_one, table_two)
            grid_low, misfit = grid_frames(kspace, blocks_used, row_offset, col_offset, row_first, col_first, row_taps, col_taps, measured)
            partial_image = coil_adjoint(grid_low, maps, table_one, table_two)
            return ((grad_sum + partial_image, misfit_sum + misfit), None)
        initial = (jnp.zeros(initial_image.shape, jnp.float32), jnp.zeros((FRAMES,), jnp.float32))
        totals, unused = lax.scan(per_coil, initial, (coil_maps, samples))
        return totals
    misfit_scale = 0.5 / (COILS * NB * BS)
    current = initial_image.astype(jnp.float32)
    moving = current
    momentum = 1.0
    misfit_rows = []
    for step_num in range(ITERS):
        data_grad, misfit = data_term(rounded(moving))
        misfit_rows.append(misfit * misfit_scale)
        padded = jnp.concatenate([moving[:, -1:], moving, moving[:, :1]], axis=1)
        descent = moving - step_size * (data_grad + tv_weight * cine_gradient(padded))
        updated = wavelet_prox(descent, step_size * shrink_weight)
        following = (1.0 + math.sqrt(1.0 + 4.0 * momentum * momentum)) / 2.0
        moving = updated + (momentum - 1.0) / following * (updated - current)
        current = updated
        momentum = following
    return (current, jnp.stack(misfit_rows))
```

```python
import functools
import math

import jax
import jax.numpy as jnp
import ml_dtypes
import numpy as np
from jax import lax
from jax.experimental import pallas as pl
from jax.experimental.pallas import tpu as pltpu
from jax.sharding import PartitionSpec as P

ITERS = 2
GROUP = 18
TILE = 128
ALIGN = 16
LANES = 128

step_size = 2.0
tv_weight = 0.1
smooth_floor = 0.5
shrink_weight = 0.1

F32 = jnp.float32
BF16 = jnp.bfloat16
MESH = pl.DeviceIdType.MESH


def table_pair(order):
    counter = np.arange(order)
    angle = (counter[:, None] * counter[None, :] % order) * (2.0 * math.pi / order)
    cosine = (np.cos(angle) / math.sqrt(order)).astype(ml_dtypes.bfloat16)
    sine = (np.sin(angle) / math.sqrt(order)).astype(ml_dtypes.bfloat16)
    return np.concatenate([cosine, sine], axis=1)


def partner_of(place, k, count):
    if count & (count - 1):
        return lax.rem(place + k, count)
    result, bit = 0, 1
    while bit < count:
        digit = place // bit % 2
        result = result + (1 - digit if k & bit else digit) * bit
        bit *= 2
    return result


def owner_of(place, k, count):
    if count & (count - 1):
        return lax.rem(place + count - k, count)
    return partner_of(place, k, count)


def dot(left, right):
    return jnp.dot(left, right, preferred_element_type=F32)


def dot_nt(left, right):
    return lax.dot_general(left, right, (((1,), (1,)), ((), ())), preferred_element_type=F32)


def partner(values, axis, parity):
    size = values.shape[axis]
    return jnp.where(
        parity == 0, pltpu.roll(values, size - 1, axis), pltpu.roll(values, 1, axis)
    )


def shrink_pair(real, imag, limit):
    length = jnp.sqrt(real * real + imag * imag)
    factor = jnp.maximum(length - limit, 0.0) / jnp.maximum(length, limit)
    return real * factor, imag * factor


def wavelet_prox(fields, limit):
    shape = fields[0].shape
    row_parity = lax.broadcasted_iota(jnp.int32, shape, 0) % 2
    col_parity = lax.broadcasted_iota(jnp.int32, shape, 1) % 2
    row_sign = jnp.where(row_parity == 0, 1.0, -1.0)
    col_sign = jnp.where(col_parity == 0, 1.0, -1.0)
    parts = []
    for field in fields:
        beside = partner(field, 1, col_parity)
        col_sum = field + beside
        col_diff = (field - beside) * col_sign
        sum_below = partner(col_sum, 0, row_parity)
        diff_below = partner(col_diff, 0, row_parity)
        approx = (col_sum + sum_below) * 0.5
        horiz = (col_diff + diff_below) * 0.5
        vertical = (col_sum - sum_below) * row_sign * 0.5
        diagonal = (col_diff - diff_below) * row_sign * 0.5
        parts.append((approx, horiz, vertical, diagonal))
    real, imag = parts
    horiz = shrink_pair(real[1], imag[1], limit)
    vertical = shrink_pair(real[2], imag[2], limit)
    diagonal = shrink_pair(real[3], imag[3], limit)
    return [
        (parts[p][0] + col_sign * horiz[p] + row_sign * vertical[p] + row_sign * col_sign * diagonal[p])
        for p in range(2)
    ]


def kernel(
    coils,
    frames,
    *refs,
):
    inputs = refs[:11]
    image_ref, misfit_ref = refs[11:13]
    held = refs[13:24]
    input_sem = refs[24]
    loads = []
    for place, (source, target) in enumerate(zip(inputs, held)):
        copy = pltpu.make_async_copy(source, target, input_sem.at[place])
        copy.start()
        loads.append(copy)
    run(coils, frames, loads, *held, image_ref, misfit_ref, *refs[25:])


def run(
    coils,
    frames,
    loads,
    start_ref,
    maps_ref,
    samples_ref,
    used_ref,
    row_off_ref,
    col_off_ref,
    row_first_ref,
    col_first_ref,
    row_taps_ref,
    col_taps_ref,
    table_ref,
    image_ref,
    misfit_ref,
    forward_ref,
    inverse_ref,
    row_ref,
    col_ref,
    stack_ref,
    space_ref,
    grid_ref,
    grad_ref,
    moving_ref,
    current_ref,
    low_ref,
    gather_ref,
    outgo_ref,
    income_ref,
    beside_ref,
    tally_ref,
    tallies_ref,
    gather_send,
    gather_recv,
    income_send,
    income_recv,
    beside_send,
    beside_recv,
    tally_send,
    tally_recv,
):
    coil = lax.axis_index("coil")
    frame = lax.axis_index("frame")
    size = maps_ref.shape[2]
    blocks = samples_ref.shape[2]
    spoke = samples_ref.shape[4]
    taps = row_taps_ref.shape[2]
    rows = size // coils
    later = lax.rem(frame + 1, frames)
    earlier = lax.rem(frame + frames - 1, frames)
    peers = [partner_of(coil, k, coils) for k in range(coils)]
    owners = [owner_of(coil, k, coils) for k in range(coils)]
    order = list(range(coils - 1, 0, -1))
    wire = gather_ref.dtype

    barrier = pltpu.get_barrier_semaphore()
    for k in range(1, coils):
        pl.semaphore_signal(barrier, inc=1, device_id={"coil": peers[k]}, device_id_type=MESH)
    for nearby in (later, earlier):
        pl.semaphore_signal(barrier, inc=1, device_id={"frame": nearby}, device_id_type=MESH)
    loads[0].wait()
    for p in range(2):
        value = start_ref[:, 0, p, :]
        low_ref[0, p] = value.astype(BF16).astype(wire)
        moving_ref[0, p] = value
        current_ref[p] = value
    pl.semaphore_wait(barrier, coils - 1 + 2)

    pending = []

    def send(source, target, send_sem, recv_sem, where):
        copy = pltpu.make_async_remote_copy(
            src_ref=source,
            dst_ref=target,
            send_sem=send_sem,
            recv_sem=recv_sem,
            device_id=where,
            device_id_type=MESH,
        )
        copy.start()
        pending.append(copy)
        return copy

    def spread_image(it, low, full):
        gathers = {
            k: send(low, gather_ref.at[it, k], gather_send.at[it, k], gather_recv.at[it, k], {"coil": peers[k]})
            for k in order
        }
        besides = [
            send(full, beside_ref.at[it, side], beside_send.at[it, side], beside_recv.at[it, side], {"frame": where})
            for side, where in ((0, later), (1, earlier))
        ]
        return gathers, besides

    gathers, besides = spread_image(0, low_ref.at[0], moving_ref.at[0])

    for place in range(4, 10):
        loads[place].wait()
    loads[10].wait()
    cosine = table_ref[:, :size]
    sine = table_ref[:, size:]
    forward_ref[:size, :size] = cosine
    forward_ref[:size, size:] = -sine
    forward_ref[size:, :size] = sine
    forward_ref[size:, size:] = cosine
    inverse_ref[:size, :size] = cosine
    inverse_ref[:size, size:] = sine
    inverse_ref[size:, :size] = -sine
    inverse_ref[size:, size:] = cosine

    strip = 64
    strips = size // ALIGN
    group = max(d for d in range(1, GROUP + 1) if blocks % d == 0)

    def build(block, carry):
        for first_ref, off_ref, taps_ref, into_ref in (
            (row_first_ref, row_off_ref, row_taps_ref, row_ref),
            (col_first_ref, col_off_ref, col_taps_ref, col_ref),
        ):
            first = first_ref[block] + off_ref[0, block]
            weights = taps_ref[0, block].astype(F32)
            for low in range(0, size, strip):
                distance = lax.broadcasted_iota(jnp.int32, (strip, spoke), 0) + low - first
                matrix = jnp.zeros((strip, spoke), F32)
                for tap in range(taps):
                    matrix = jnp.where(distance == tap, weights[tap : tap + 1], matrix)
                matrix = matrix.astype(BF16)
                if into_ref is col_ref:
                    into_ref[block, low : low + strip, :] = matrix
                else:
                    into_ref[block, low // ALIGN : (low + strip) // ALIGN] = matrix.reshape(-1, ALIGN, spoke)
        row_ref[block, strips] = jnp.zeros((ALIGN, spoke), BF16)
        return carry

    lax.fori_loop(0, blocks, build, 0)
    tally_ref[...] = jnp.zeros_like(tally_ref)
    for p in range(2):
        space_ref[p, strips] = jnp.zeros((ALIGN, size), BF16)
    window = TILE // ALIGN + 1
    deep = window * ALIGN
    for place in range(1, 4):
        loads[place].wait()
    used = used_ref[0, 0]
    momentum = 1.0

    for it in range(ITERS):
        for k in [0] + order[::-1]:
            if k == 0:
                piece = low_ref[it]
            else:
                gathers[k].wait_recv()
                piece = gather_ref[it, k]
            piece = piece.astype(F32)
            owner = owners[k]
            at = pl.multiple_of(owner * rows, rows)
            at_below = pl.multiple_of(owner * rows + size, rows)
            map_real = maps_ref[0, 0, pl.ds(at, rows), :].astype(F32)
            map_imag = maps_ref[0, 1, pl.ds(at, rows), :].astype(F32)
            real = (map_real * piece[0] - map_imag * piece[1]).astype(BF16).astype(wire)
            imag = (map_real * piece[1] + map_imag * piece[0]).astype(BF16).astype(wire)
            stack_ref[pl.ds(at, rows), :size] = real
            stack_ref[pl.ds(at, rows), size:] = imag
            stack_ref[pl.ds(at_below, rows), :size] = imag
            stack_ref[pl.ds(at_below, rows), size:] = -real
        half = dot(table_ref[...], stack_ref[...].astype(BF16)).astype(BF16)
        kspace = dot(half, forward_ref[...]).astype(BF16)
        for p in range(2):
            space_ref[p, :strips] = kspace[:, p * size : (p + 1) * size].reshape(strips, ALIGN, size)
        grid_ref[...] = jnp.zeros_like(grid_ref)

        def predict(turn, total):
            lows = []
            for member in range(group):
                block = turn * group + member
                at = lax.div(row_off_ref[0, block], ALIGN)
                near = jnp.concatenate([space_ref[p, at + i] for p in range(2) for i in range(window)], axis=0)
                across = dot(near, col_ref[block])
                rows_wide = jnp.concatenate([row_ref[block, at + i] for i in range(window)], axis=0).astype(F32)
                measured = samples_ref[0, 0, block].astype(F32)
                active = jnp.where(block < used, 1.0, 0.0)
                for p in range(2):
                    predicted = jnp.sum(
                        across[p * deep : (p + 1) * deep] * rows_wide, axis=0, keepdims=True
                    )
                    resid = (predicted - measured[p : p + 1]) * active
                    total = total + resid * resid
                    lows.append(resid)
            return total, tuple(lows)

        def spread(turn, lows):
            left, sides = ([], []), []
            for member in range(group):
                block = turn * group + member
                sides.append(col_ref[block])
                rows_wide = row_ref[block, :strips].reshape(size, spoke)
                for p in range(2):
                    left[p].append(lows[2 * member + p].astype(BF16) * rows_wide)
            both = jnp.concatenate([jnp.concatenate(part, axis=1) for part in left], axis=0)
            grid_ref[...] += dot_nt(both, jnp.concatenate(sides, axis=1))

        def visit(turn, carry):
            total, lows = carry
            spread(turn - 1, lows)
            return predict(turn, total)

        turns = blocks // group
        carry = predict(0, jnp.zeros((1, spoke), F32))
        total, lows = lax.fori_loop(1, turns, visit, carry) if turns > 1 else carry
        spread(turns - 1, lows)
        tally_ref[it : it + 1, :] = total
        tally_copies = []
        if it == ITERS - 1:
            tally_copies = [
                send(tally_ref, tallies_ref.at[k], tally_send.at[k], tally_recv.at[k], {"coil": peers[k]})
                for k in range(1, coils)
            ]
        grid_real = grid_ref[:size].astype(BF16)
        grid_imag = grid_ref[size:].astype(BF16)
        turned = jnp.concatenate(
            [
                jnp.concatenate([grid_real, grid_imag], axis=1),
                jnp.concatenate([-grid_imag, grid_real], axis=1),
            ],
            axis=0,
        )
        back_half = dot(table_ref[...], turned).astype(BF16)
        coil_back = dot(back_half, inverse_ref[...])
        map_real = maps_ref[0, 0].astype(F32)
        map_imag = maps_ref[0, 1].astype(F32)
        back_real = coil_back[:, :size]
        back_imag = coil_back[:, size:]
        real = map_real * back_real + map_imag * back_imag
        imag = map_real * back_imag - map_imag * back_real
        outgo_ref[it, 0] = real.astype(wire)
        outgo_ref[it, 1] = imag.astype(wire)
        incomes = {}
        for k in order:
            at = pl.multiple_of(peers[k] * rows, rows)
            incomes[k] = send(
                outgo_ref.at[it, :, pl.ds(at, rows), :],
                income_ref.at[it, k],
                income_send.at[it, k],
                income_recv.at[it, k],
                {"coil": peers[k]},
            )
        grad_ref[0] = real
        grad_ref[1] = imag

        for copy in besides:
            copy.wait_recv()
        moving = [moving_ref[it, p] for p in range(2)]
        ahead = [beside_ref[it, 1, p] - moving[p] for p in range(2)]
        behind = [moving[p] - beside_ref[it, 0, p] for p in range(2)]
        floor = smooth_floor * smooth_floor
        ahead_length = jnp.sqrt(ahead[0] * ahead[0] + ahead[1] * ahead[1] + floor)
        behind_length = jnp.sqrt(behind[0] * behind[0] + behind[1] * behind[1] + floor)
        variation = [behind[p] / behind_length - ahead[p] / ahead_length for p in range(2)]

        here = pl.multiple_of(coil * rows, rows)
        sums = [grad_ref[p, pl.ds(here, rows), :] for p in range(2)]
        for k in range(1, coils):
            incomes[k].wait_recv()
            sums = [sums[p] + income_ref[it, k, p].astype(F32) for p in range(2)]
        descent = [moving[p] - step_size * (sums[p] + tv_weight * variation[p]) for p in range(2)]
        doubled = wavelet_prox(descent, step_size * shrink_weight)
        updated = [doubled[p] * 0.5 for p in range(2)]
        following = (1.0 + math.sqrt(1.0 + 4.0 * momentum * momentum)) / 2.0
        if it == ITERS - 1:
            tiles = size // LANES
            for p in range(2):
                for tile in range(tiles):
                    image_ref[pl.ds(2 * tile + p, rows, stride=2 * tiles), :] = doubled[p][
                        :, tile * LANES : (tile + 1) * LANES
                    ]
        else:
            factor = (momentum - 1.0) / following
            for p in range(2):
                ahead_value = updated[p]
                if factor != 0.0:
                    ahead_value = ahead_value + factor * (updated[p] - current_ref[p])
                low_ref[it + 1, p] = ahead_value.astype(BF16).astype(wire)
                moving_ref[it + 1, p] = ahead_value
                current_ref[p] = updated[p]
            gathers, besides = spread_image(it + 1, low_ref.at[it + 1], moving_ref.at[it + 1])
        momentum = following

    tally = tally_ref[...]
    for k in range(1, coils):
        tally_copies[k - 1].wait_recv()
        tally = tally + tallies_ref[k]
    lane = lax.broadcasted_iota(jnp.int32, (1, ITERS), 1)
    misfit = jnp.zeros((1, ITERS), F32)
    for it in range(ITERS):
        misfit = jnp.where(lane == it, jnp.sum(tally[it : it + 1], axis=1, keepdims=True), misfit)
    misfit_ref[...] = misfit
    for copy in pending:
        copy.wait_send()


def on_device(coils, frames, table, image, coil_maps, samples, blocks_used, row_off, col_off, row_first, col_first, *taps):
    size = coil_maps.shape[3]
    blocks = samples.shape[2]
    spoke = samples.shape[4]
    rows = size // coils
    wire = BF16 if rows % 16 == 0 else F32
    row_first = jnp.transpose(row_first, (1, 0, 2))
    col_first = jnp.transpose(col_first, (1, 0, 2))
    vmem = pl.BlockSpec(memory_space=pltpu.VMEM)
    operands = (
        image,
        coil_maps,
        samples,
        blocks_used.reshape(1, 1),
        row_off,
        col_off,
        row_first,
        col_first,
        *taps,
        table,
    )
    scalars = (3, 4, 5)
    held = [
        (pltpu.SMEM if place in scalars else pltpu.VMEM)(operand.shape, operand.dtype)
        for place, operand in enumerate(operands)
    ]
    shard = (2, rows, size)
    dma = pltpu.SemaphoreType.DMA
    doubled, misfit = pl.pallas_call(
        functools.partial(kernel, coils, frames),
        out_shape=(
            pltpu.VMEM((2 * rows * size // LANES, LANES), F32),
            pltpu.VMEM((1, ITERS), F32),
        ),
        in_specs=[pl.BlockSpec(memory_space=pl.ANY)] * len(operands),
        out_specs=(vmem, vmem),
        scratch_shapes=held
        + [
            dma((len(operands),)),
            pltpu.VMEM((2 * size, 2 * size), BF16),
            pltpu.VMEM((2 * size, 2 * size), BF16),
            pltpu.VMEM((blocks, size // ALIGN + 1, ALIGN, spoke), BF16),
            pltpu.VMEM((blocks, size, spoke), BF16),
            pltpu.VMEM((2 * size, 2 * size), wire),
            pltpu.VMEM((2, size // ALIGN + 1, ALIGN, size), BF16),
            pltpu.VMEM((2 * size, size), F32),
            pltpu.VMEM((2, size, size), F32),
            pltpu.VMEM((ITERS,) + shard, F32),
            pltpu.VMEM(shard, F32),
            pltpu.VMEM((ITERS,) + shard, wire),
            pltpu.VMEM((ITERS, coils) + shard, wire),
            pltpu.VMEM((ITERS, 2, size, size), wire),
            pltpu.VMEM((ITERS, coils) + shard, wire),
            pltpu.VMEM((ITERS, 2) + shard, F32),
            pltpu.VMEM((8, spoke), F32),
            pltpu.VMEM((coils, 8, spoke), F32),
            dma((ITERS, coils)),
            dma((ITERS, coils)),
            dma((ITERS, coils)),
            dma((ITERS, coils)),
            dma((ITERS, 2)),
            dma((ITERS, 2)),
            dma((coils,)),
            dma((coils,)),
        ],
        compiler_params=pltpu.CompilerParams(
            collective_id=0, has_side_effects=True, vmem_limit_bytes=56 * 1024 * 1024
        ),
    )(*operands)
    updated = (doubled * 0.5).reshape(rows, size // LANES, 2, LANES).transpose(0, 2, 1, 3)
    scale = 0.5 / (coils * blocks * spoke)
    return updated.reshape(image.shape), jnp.transpose(misfit * scale)


def solution(mesh):
    placed = (
        P("coil", "frame", None, None),
        P("coil", None, None, None),
        P("coil", "frame", None, None, None),
        P("frame"),
        P("frame", None),
        P("frame", None),
        P("frame", None, None),
        P("frame", None, None),
        P("frame", None, None, None),
        P("frame", None, None, None),
    )

    def run(*args):
        table = jnp.asarray(table_pair(args[1].shape[3]))
        body = functools.partial(on_device, mesh.shape["coil"], mesh.shape["frame"], table)
        return jax.shard_map(
            body,
            mesh=mesh,
            in_specs=placed,
            out_specs=(P("coil", "frame", None, None), P(None, "frame")),
            check_vma=False,
        )(*args)

    return run
```

```python
import functools
import math

import jax
import jax.numpy as jnp
import ml_dtypes
import numpy as np
from jax import lax
from jax.experimental import pallas as pl
from jax.experimental.pallas import tpu as pltpu
from jax.sharding import PartitionSpec as P

ITERS = 2
GROUP = 18
TILE = 128
ALIGN = 16
LANES = 128
LEAD = 3
HOLD = (0, 1, 2, )

step_size = 2.0
tv_weight = 0.1
smooth_floor = 0.5
shrink_weight = 0.1

F32 = jnp.float32
BF16 = jnp.bfloat16
MESH = pl.DeviceIdType.MESH


def table_pair(order):
    counter = np.arange(order)
    angle = (counter[:, None] * counter[None, :] % order) * (2.0 * math.pi / order)
    cosine = (np.cos(angle) / math.sqrt(order)).astype(ml_dtypes.bfloat16)
    sine = (np.sin(angle) / math.sqrt(order)).astype(ml_dtypes.bfloat16)
    return np.concatenate([cosine, sine], axis=1)


def partner_of(place, k, count):
    if count & (count - 1):
        return lax.rem(place + k, count)
    result, bit = 0, 1
    while bit < count:
        digit = place // bit % 2
        result = result + (1 - digit if k & bit else digit) * bit
        bit *= 2
    return result


def owner_of(place, k, count):
    if count & (count - 1):
        return lax.rem(place + count - k, count)
    return partner_of(place, k, count)


def dot(left, right):
    return jnp.dot(left, right, preferred_element_type=F32)


def dot_nt(left, right):
    return lax.dot_general(left, right, (((1,), (1,)), ((), ())), preferred_element_type=F32)


def partner(values, axis, parity):
    size = values.shape[axis]
    return jnp.where(
        parity == 0, pltpu.roll(values, size - 1, axis), pltpu.roll(values, 1, axis)
    )


def shrink_pair(real, imag, limit):
    length = jnp.sqrt(real * real + imag * imag)
    factor = jnp.maximum(length - limit, 0.0) / jnp.maximum(length, limit)
    return real * factor, imag * factor


def wavelet_prox(fields, limit):
    shape = fields[0].shape
    row_parity = lax.broadcasted_iota(jnp.int32, shape, 0) % 2
    col_parity = lax.broadcasted_iota(jnp.int32, shape, 1) % 2
    row_sign = jnp.where(row_parity == 0, 1.0, -1.0)
    col_sign = jnp.where(col_parity == 0, 1.0, -1.0)
    parts = []
    for field in fields:
        beside = partner(field, 1, col_parity)
        col_sum = field + beside
        col_diff = (field - beside) * col_sign
        sum_below = partner(col_sum, 0, row_parity)
        diff_below = partner(col_diff, 0, row_parity)
        approx = (col_sum + sum_below) * 0.5
        horiz = (col_diff + diff_below) * 0.5
        vertical = (col_sum - sum_below) * row_sign * 0.5
        diagonal = (col_diff - diff_below) * row_sign * 0.5
        parts.append((approx, horiz, vertical, diagonal))
    real, imag = parts
    horiz = shrink_pair(real[1], imag[1], limit)
    vertical = shrink_pair(real[2], imag[2], limit)
    diagonal = shrink_pair(real[3], imag[3], limit)
    return [
        (parts[p][0] + col_sign * horiz[p] + row_sign * vertical[p] + row_sign * col_sign * diagonal[p])
        for p in range(2)
    ]


def kernel(
    coils,
    frames,
    *refs,
):
    inputs = refs[:11]
    image_ref, misfit_ref = refs[11:13]
    held = refs[13:24]
    input_sem = refs[24]
    loads = []
    for place, (source, target) in enumerate(zip(inputs, held)):
        copy = pltpu.make_async_copy(source, target, input_sem.at[place])
        copy.start()
        loads.append(copy)
    run(coils, frames, loads, *held, image_ref, misfit_ref, *refs[25:])


def run(
    coils,
    frames,
    loads,
    start_ref,
    maps_ref,
    samples_ref,
    used_ref,
    row_off_ref,
    col_off_ref,
    row_first_ref,
    col_first_ref,
    row_taps_ref,
    col_taps_ref,
    table_ref,
    image_ref,
    misfit_ref,
    forward_ref,
    inverse_ref,
    row_ref,
    col_ref,
    stack_ref,
    space_ref,
    grid_ref,
    grad_ref,
    moving_ref,
    current_ref,
    low_ref,
    gather_ref,
    outgo_ref,
    income_ref,
    beside_ref,
    tally_ref,
    tallies_ref,
    gather_send,
    gather_recv,
    income_send,
    income_recv,
    beside_send,
    beside_recv,
    tally_send,
    tally_recv,
    turn_sem,
):
    coil = lax.axis_index("coil")
    frame = lax.axis_index("frame")
    size = maps_ref.shape[2]
    blocks = samples_ref.shape[2]
    spoke = samples_ref.shape[4]
    taps = row_taps_ref.shape[2]
    rows = size // coils
    later = lax.rem(frame + 1, frames)
    earlier = lax.rem(frame + frames - 1, frames)
    peers = [partner_of(coil, k, coils) for k in range(coils)]
    owners = [owner_of(coil, k, coils) for k in range(coils)]
    order = list(range(coils - 1, 0, -1))
    wire = gather_ref.dtype

    barrier = pltpu.get_barrier_semaphore()
    for k in range(1, coils):
        pl.semaphore_signal(barrier, inc=1, device_id={"coil": peers[k]}, device_id_type=MESH)
    for nearby in (later, earlier):
        pl.semaphore_signal(barrier, inc=1, device_id={"frame": nearby}, device_id_type=MESH)
    loads[0].wait()
    for p in range(2):
        value = start_ref[:, 0, p, :]
        low_ref[0, p] = value.astype(BF16).astype(wire)
        moving_ref[0, p] = value
        current_ref[p] = value
    pl.semaphore_wait(barrier, coils - 1 + 2)

    pending = []

    def send(source, target, send_sem, recv_sem, where):
        copy = pltpu.make_async_remote_copy(
            src_ref=source,
            dst_ref=target,
            send_sem=send_sem,
            recv_sem=recv_sem,
            device_id=where,
            device_id_type=MESH,
        )
        pending.append(copy)
        return copy

    paired = frames % 2 == 0
    sibling = frame + 1 - 2 * lax.rem(frame, 2)
    first_core = lax.rem(frame, 2) == 0

    def start(phase, copies):
        if paired and phase in HOLD:
            pl.when(jnp.logical_not(first_core))(lambda: pl.semaphore_wait(turn_sem.at[phase], 1))
        for copy in copies:
            copy.start()

    def sent(phase, copies):
        if paired and phase in HOLD:
            for copy in copies:
                pending[:] = [one for one in pending if one is not copy]

            @pl.when(first_core)
            def _():
                for copy in copies[:LEAD]:
                    copy.wait_send()
                pl.semaphore_signal(turn_sem.at[phase], inc=1, device_id={"frame": sibling}, device_id_type=MESH)
                for copy in copies[LEAD:]:
                    copy.wait_send()

            held_back.extend(copies)

    held_back = []

    def spread_image(it, low, full):
        gathers = {
            k: send(low, gather_ref.at[it, k], gather_send.at[it, k], gather_recv.at[it, k], {"coil": peers[k]})
            for k in order
        }
        besides = [
            send(full, beside_ref.at[it, side], beside_send.at[it, side], beside_recv.at[it, side], {"frame": where})
            for side, where in ((0, later), (1, earlier))
        ]
        return gathers, besides

    gathers, besides = spread_image(0, low_ref.at[0], moving_ref.at[0])
    start(0, list(gathers.values()) + besides)

    for place in range(4, 10):
        loads[place].wait()
    loads[10].wait()
    cosine = table_ref[:, :size]
    sine = table_ref[:, size:]
    forward_ref[:size, :size] = cosine
    forward_ref[:size, size:] = -sine
    forward_ref[size:, :size] = sine
    forward_ref[size:, size:] = cosine
    inverse_ref[:size, :size] = cosine
    inverse_ref[:size, size:] = sine
    inverse_ref[size:, :size] = -sine
    inverse_ref[size:, size:] = cosine

    strip = 64
    strips = size // ALIGN
    group = max(d for d in range(1, GROUP + 1) if blocks % d == 0)

    def build(block, carry):
        for first_ref, off_ref, taps_ref, into_ref in (
            (row_first_ref, row_off_ref, row_taps_ref, row_ref),
            (col_first_ref, col_off_ref, col_taps_ref, col_ref),
        ):
            first = first_ref[block] + off_ref[0, block]
            weights = taps_ref[0, block].astype(F32)
            for low in range(0, size, strip):
                distance = lax.broadcasted_iota(jnp.int32, (strip, spoke), 0) + low - first
                matrix = jnp.zeros((strip, spoke), F32)
                for tap in range(taps):
                    matrix = jnp.where(distance == tap, weights[tap : tap + 1], matrix)
                matrix = matrix.astype(BF16)
                if into_ref is col_ref:
                    into_ref[block, low : low + strip, :] = matrix
                else:
                    into_ref[block, low // ALIGN : (low + strip) // ALIGN] = matrix.reshape(-1, ALIGN, spoke)
        row_ref[block, strips] = jnp.zeros((ALIGN, spoke), BF16)
        return carry

    lax.fori_loop(0, blocks, build, 0)
    tally_ref[...] = jnp.zeros_like(tally_ref)
    for p in range(2):
        space_ref[p, strips] = jnp.zeros((ALIGN, size), BF16)
    window = TILE // ALIGN + 1
    deep = window * ALIGN
    for place in range(1, 4):
        loads[place].wait()
    sent(0, list(gathers.values()))
    used = used_ref[0, 0]
    momentum = 1.0

    for it in range(ITERS):
        for k in [0] + order[::-1]:
            if k == 0:
                piece = low_ref[it]
            else:
                gathers[k].wait_recv()
                piece = gather_ref[it, k]
            piece = piece.astype(F32)
            owner = owners[k]
            at = pl.multiple_of(owner * rows, rows)
            at_below = pl.multiple_of(owner * rows + size, rows)
            map_real = maps_ref[0, 0, pl.ds(at, rows), :].astype(F32)
            map_imag = maps_ref[0, 1, pl.ds(at, rows), :].astype(F32)
            real = (map_real * piece[0] - map_imag * piece[1]).astype(BF16).astype(wire)
            imag = (map_real * piece[1] + map_imag * piece[0]).astype(BF16).astype(wire)
            stack_ref[pl.ds(at, rows), :size] = real
            stack_ref[pl.ds(at, rows), size:] = imag
            stack_ref[pl.ds(at_below, rows), :size] = imag
            stack_ref[pl.ds(at_below, rows), size:] = -real
        half = dot(table_ref[...], stack_ref[...].astype(BF16)).astype(BF16)
        kspace = dot(half, forward_ref[...]).astype(BF16)
        for p in range(2):
            space_ref[p, :strips] = kspace[:, p * size : (p + 1) * size].reshape(strips, ALIGN, size)
        grid_ref[...] = jnp.zeros_like(grid_ref)

        def predict(turn, total):
            lows = []
            for member in range(group):
                block = turn * group + member
                at = lax.div(row_off_ref[0, block], ALIGN)
                near = jnp.concatenate([space_ref[p, at + i] for p in range(2) for i in range(window)], axis=0)
                across = dot(near, col_ref[block])
                rows_wide = jnp.concatenate([row_ref[block, at + i] for i in range(window)], axis=0).astype(F32)
                measured = samples_ref[0, 0, block].astype(F32)
                active = jnp.where(block < used, 1.0, 0.0)
                for p in range(2):
                    predicted = jnp.sum(
                        across[p * deep : (p + 1) * deep] * rows_wide, axis=0, keepdims=True
                    )
                    resid = (predicted - measured[p : p + 1]) * active
                    total = total + resid * resid
                    lows.append(resid)
            return total, tuple(lows)

        def spread(turn, lows):
            left, sides = ([], []), []
            for member in range(group):
                block = turn * group + member
                sides.append(col_ref[block])
                rows_wide = row_ref[block, :strips].reshape(size, spoke)
                for p in range(2):
                    left[p].append(lows[2 * member + p].astype(BF16) * rows_wide)
            side = jnp.concatenate(sides, axis=1)
            for p in range(2):
                grid_ref[p * size : (p + 1) * size] += dot_nt(jnp.concatenate(left[p], axis=1), side)

        def visit(turn, carry):
            total, lows = carry
            spread(turn - 1, lows)
            return predict(turn, total)

        turns = blocks // group
        carry = predict(0, jnp.zeros((1, spoke), F32))
        total, lows = lax.fori_loop(1, turns, visit, carry) if turns > 1 else carry
        spread(turns - 1, lows)
        tally_ref[it : it + 1, :] = total
        grid_real = grid_ref[:size].astype(BF16)
        grid_imag = grid_ref[size:].astype(BF16)
        turned = jnp.concatenate(
            [
                jnp.concatenate([grid_real, grid_imag], axis=1),
                jnp.concatenate([-grid_imag, grid_real], axis=1),
            ],
            axis=0,
        )
        back_half = dot(table_ref[...], turned).astype(BF16)
        coil_back = dot(back_half, inverse_ref[...])
        map_real = maps_ref[0, 0].astype(F32)
        map_imag = maps_ref[0, 1].astype(F32)
        back_real = coil_back[:, :size]
        back_imag = coil_back[:, size:]
        real = map_real * back_real + map_imag * back_imag
        imag = map_real * back_imag - map_imag * back_real
        outgo_ref[it, 0] = real.astype(wire)
        outgo_ref[it, 1] = imag.astype(wire)
        incomes = {}
        for k in order:
            at = pl.multiple_of(peers[k] * rows, rows)
            incomes[k] = send(
                outgo_ref.at[it, :, pl.ds(at, rows), :],
                income_ref.at[it, k],
                income_send.at[it, k],
                income_recv.at[it, k],
                {"coil": peers[k]},
            )
        start(2 * it + 1, incomes.values())
        tally_copies = []
        if it == ITERS - 1:
            tally_copies = [
                send(tally_ref, tallies_ref.at[k], tally_send.at[k], tally_recv.at[k], {"coil": peers[k]})
                for k in range(1, coils)
            ]
            for copy in tally_copies:
                copy.start()
        grad_ref[0] = real
        grad_ref[1] = imag

        for copy in besides:
            copy.wait_recv()
        moving = [moving_ref[it, p] for p in range(2)]
        ahead = [beside_ref[it, 1, p] - moving[p] for p in range(2)]
        behind = [moving[p] - beside_ref[it, 0, p] for p in range(2)]
        floor = smooth_floor * smooth_floor
        ahead_length = jnp.sqrt(ahead[0] * ahead[0] + ahead[1] * ahead[1] + floor)
        behind_length = jnp.sqrt(behind[0] * behind[0] + behind[1] * behind[1] + floor)
        variation = [behind[p] / behind_length - ahead[p] / ahead_length for p in range(2)]

        sent(2 * it + 1, list(incomes.values()))
        here = pl.multiple_of(coil * rows, rows)
        sums = [grad_ref[p, pl.ds(here, rows), :] for p in range(2)]
        for k in range(1, coils):
            incomes[k].wait_recv()
            sums = [sums[p] + income_ref[it, k, p].astype(F32) for p in range(2)]
        descent = [moving[p] - step_size * (sums[p] + tv_weight * variation[p]) for p in range(2)]
        doubled = wavelet_prox(descent, step_size * shrink_weight)
        updated = [doubled[p] * 0.5 for p in range(2)]
        following = (1.0 + math.sqrt(1.0 + 4.0 * momentum * momentum)) / 2.0
        if it == ITERS - 1:
            tiles = size // LANES
            for p in range(2):
                for tile in range(tiles):
                    image_ref[pl.ds(2 * tile + p, rows, stride=2 * tiles), :] = doubled[p][
                        :, tile * LANES : (tile + 1) * LANES
                    ]
        else:
            factor = (momentum - 1.0) / following
            for p in range(2):
                ahead_value = updated[p]
                if factor != 0.0:
                    ahead_value = ahead_value + factor * (updated[p] - current_ref[p])
                low_ref[it + 1, p] = ahead_value.astype(BF16).astype(wire)
                moving_ref[it + 1, p] = ahead_value
                current_ref[p] = updated[p]
            gathers, besides = spread_image(it + 1, low_ref.at[it + 1], moving_ref.at[it + 1])
            start(2 * it + 2, list(gathers.values()) + besides)
            sent(2 * it + 2, list(gathers.values()))
        momentum = following

    tally = tally_ref[...]
    for k in range(1, coils):
        tally_copies[k - 1].wait_recv()
        tally = tally + tallies_ref[k]
    lane = lax.broadcasted_iota(jnp.int32, (1, ITERS), 1)
    misfit = jnp.zeros((1, ITERS), F32)
    for it in range(ITERS):
        misfit = jnp.where(lane == it, jnp.sum(tally[it : it + 1], axis=1, keepdims=True), misfit)
    misfit_ref[...] = misfit
    for copy in pending:
        copy.wait_send()
    if held_back:

        @pl.when(jnp.logical_not(first_core))
        def _():
            for copy in held_back:
                copy.wait_send()


def on_device(coils, frames, table, image, coil_maps, samples, blocks_used, row_off, col_off, row_first, col_first, *taps):
    size = coil_maps.shape[3]
    blocks = samples.shape[2]
    spoke = samples.shape[4]
    rows = size // coils
    wire = BF16 if rows % 16 == 0 else F32
    row_first = jnp.transpose(row_first, (1, 0, 2))
    col_first = jnp.transpose(col_first, (1, 0, 2))
    vmem = pl.BlockSpec(memory_space=pltpu.VMEM)
    operands = (
        image,
        coil_maps,
        samples,
        blocks_used.reshape(1, 1),
        row_off,
        col_off,
        row_first,
        col_first,
        *taps,
        table,
    )
    scalars = (3, 4, 5)
    held = [
        (pltpu.SMEM if place in scalars else pltpu.VMEM)(operand.shape, operand.dtype)
        for place, operand in enumerate(operands)
    ]
    shard = (2, rows, size)
    dma = pltpu.SemaphoreType.DMA
    doubled, misfit = pl.pallas_call(
        functools.partial(kernel, coils, frames),
        out_shape=(
            pltpu.VMEM((2 * rows * size // LANES, LANES), F32),
            pltpu.VMEM((1, ITERS), F32),
        ),
        in_specs=[pl.BlockSpec(memory_space=pl.ANY)] * len(operands),
        out_specs=(vmem, vmem),
        scratch_shapes=held
        + [
            dma((len(operands),)),
            pltpu.VMEM((2 * size, 2 * size), BF16),
            pltpu.VMEM((2 * size, 2 * size), BF16),
            pltpu.VMEM((blocks, size // ALIGN + 1, ALIGN, spoke), BF16),
            pltpu.VMEM((blocks, size, spoke), BF16),
            pltpu.VMEM((2 * size, 2 * size), wire),
            pltpu.VMEM((2, size // ALIGN + 1, ALIGN, size), BF16),
            pltpu.VMEM((2 * size, size), F32),
            pltpu.VMEM((2, size, size), F32),
            pltpu.VMEM((ITERS,) + shard, F32),
            pltpu.VMEM(shard, F32),
            pltpu.VMEM((ITERS,) + shard, wire),
            pltpu.VMEM((ITERS, coils) + shard, wire),
            pltpu.VMEM((ITERS, 2, size, size), wire),
            pltpu.VMEM((ITERS, coils) + shard, wire),
            pltpu.VMEM((ITERS, 2) + shard, F32),
            pltpu.VMEM((8, spoke), F32),
            pltpu.VMEM((coils, 8, spoke), F32),
            dma((ITERS, coils)),
            dma((ITERS, coils)),
            dma((ITERS, coils)),
            dma((ITERS, coils)),
            dma((ITERS, 2)),
            dma((ITERS, 2)),
            dma((coils,)),
            dma((coils,)),
            pltpu.SemaphoreType.REGULAR((2 * ITERS,)),
        ],
        compiler_params=pltpu.CompilerParams(
            collective_id=0, has_side_effects=True, vmem_limit_bytes=56 * 1024 * 1024
        ),
    )(*operands)
    updated = (doubled * 0.5).reshape(rows, size // LANES, 2, LANES).transpose(0, 2, 1, 3)
    scale = 0.5 / (coils * blocks * spoke)
    return updated.reshape(image.shape), jnp.transpose(misfit * scale)


def solution(mesh):
    placed = (
        P("coil", "frame", None, None),
        P("coil", None, None, None),
        P("coil", "frame", None, None, None),
        P("frame"),
        P("frame", None),
        P("frame", None),
        P("frame", None, None),
        P("frame", None, None),
        P("frame", None, None, None),
        P("frame", None, None, None),
    )

    def run(*args):
        table = jnp.asarray(table_pair(args[1].shape[3]))
        body = functools.partial(on_device, mesh.shape["coil"], mesh.shape["frame"], table)
        return jax.shard_map(
            body,
            mesh=mesh,
            in_specs=placed,
            out_specs=(P("coil", "frame", None, None), P(None, "frame")),
            check_vma=False,
        )(*args)

    return run
```

```python
import functools
import math

import jax
import jax.numpy as jnp
import ml_dtypes
import numpy as np
from jax import lax
from jax.experimental import pallas as pl
from jax.experimental.pallas import tpu as pltpu
from jax.sharding import PartitionSpec as P

ITERS = 2
GROUP = 18
TILE = 128
ALIGN = 16
LANES = 128
HOLD = {0: 7, 1: 3, 2: 3}

step_size = 2.0
tv_weight = 0.1
smooth_floor = 0.5
shrink_weight = 0.1

F32 = jnp.float32
BF16 = jnp.bfloat16
MESH = pl.DeviceIdType.MESH


def table_pair(order):
    counter = np.arange(order)
    angle = (counter[:, None] * counter[None, :] % order) * (2.0 * math.pi / order)
    cosine = (np.cos(angle) / math.sqrt(order)).astype(ml_dtypes.bfloat16)
    sine = (np.sin(angle) / math.sqrt(order)).astype(ml_dtypes.bfloat16)
    return np.concatenate([cosine, sine], axis=1)


def partner_of(place, k, count):
    if count & (count - 1):
        return lax.rem(place + k, count)
    result, bit = 0, 1
    while bit < count:
        digit = place // bit % 2
        result = result + (1 - digit if k & bit else digit) * bit
        bit *= 2
    return result


def owner_of(place, k, count):
    if count & (count - 1):
        return lax.rem(place + count - k, count)
    return partner_of(place, k, count)


def dot(left, right):
    return jnp.dot(left, right, preferred_element_type=F32)


def dot_nt(left, right):
    return lax.dot_general(left, right, (((1,), (1,)), ((), ())), preferred_element_type=F32)


def partner(values, axis, parity):
    size = values.shape[axis]
    return jnp.where(
        parity == 0, pltpu.roll(values, size - 1, axis), pltpu.roll(values, 1, axis)
    )


def shrink_pair(real, imag, limit):
    length = jnp.sqrt(real * real + imag * imag)
    factor = jnp.maximum(length - limit, 0.0) / jnp.maximum(length, limit)
    return real * factor, imag * factor


def wavelet_prox(fields, limit):
    shape = fields[0].shape
    row_parity = lax.broadcasted_iota(jnp.int32, shape, 0) % 2
    col_parity = lax.broadcasted_iota(jnp.int32, shape, 1) % 2
    row_sign = jnp.where(row_parity == 0, 1.0, -1.0)
    col_sign = jnp.where(col_parity == 0, 1.0, -1.0)
    parts = []
    for field in fields:
        beside = partner(field, 1, col_parity)
        col_sum = field + beside
        col_diff = (field - beside) * col_sign
        sum_below = partner(col_sum, 0, row_parity)
        diff_below = partner(col_diff, 0, row_parity)
        approx = (col_sum + sum_below) * 0.5
        horiz = (col_diff + diff_below) * 0.5
        vertical = (col_sum - sum_below) * row_sign * 0.5
        diagonal = (col_diff - diff_below) * row_sign * 0.5
        parts.append((approx, horiz, vertical, diagonal))
    real, imag = parts
    horiz = shrink_pair(real[1], imag[1], limit)
    vertical = shrink_pair(real[2], imag[2], limit)
    diagonal = shrink_pair(real[3], imag[3], limit)
    return [
        (parts[p][0] + col_sign * horiz[p] + row_sign * vertical[p] + row_sign * col_sign * diagonal[p])
        for p in range(2)
    ]


def kernel(
    coils,
    frames,
    *refs,
):
    inputs = refs[:11]
    image_ref, misfit_ref = refs[11:13]
    held = refs[13:24]
    input_sem = refs[24]
    loads = []
    for place, (source, target) in enumerate(zip(inputs, held)):
        copy = pltpu.make_async_copy(source, target, input_sem.at[place])
        copy.start()
        loads.append(copy)
    run(coils, frames, loads, *held, image_ref, misfit_ref, *refs[25:])


def run(
    coils,
    frames,
    loads,
    start_ref,
    maps_ref,
    samples_ref,
    used_ref,
    row_off_ref,
    col_off_ref,
    row_first_ref,
    col_first_ref,
    row_taps_ref,
    col_taps_ref,
    table_ref,
    image_ref,
    misfit_ref,
    forward_ref,
    inverse_ref,
    row_ref,
    col_ref,
    stack_ref,
    space_ref,
    grid_ref,
    grad_ref,
    moving_ref,
    current_ref,
    low_ref,
    gather_ref,
    outgo_ref,
    income_ref,
    beside_ref,
    tally_ref,
    tallies_ref,
    gather_send,
    gather_recv,
    income_send,
    income_recv,
    beside_send,
    beside_recv,
    tally_send,
    tally_recv,
    turn_sem,
):
    coil = lax.axis_index("coil")
    frame = lax.axis_index("frame")
    size = maps_ref.shape[2]
    blocks = samples_ref.shape[2]
    spoke = samples_ref.shape[4]
    taps = row_taps_ref.shape[2]
    rows = size // coils
    later = lax.rem(frame + 1, frames)
    earlier = lax.rem(frame + frames - 1, frames)
    peers = [partner_of(coil, k, coils) for k in range(coils)]
    owners = [owner_of(coil, k, coils) for k in range(coils)]
    order = list(range(coils - 1, 0, -1))
    wire = gather_ref.dtype
    halved = coils & (coils - 1) == 0 and coils > 1
    top = coil // max(coils // 2, 1)

    barrier = pltpu.get_barrier_semaphore()
    for k in range(1, coils):
        pl.semaphore_signal(barrier, inc=1, device_id={"coil": peers[k]}, device_id_type=MESH)
    for nearby in (later, earlier):
        pl.semaphore_signal(barrier, inc=1, device_id={"frame": nearby}, device_id_type=MESH)
    loads[0].wait()
    for p in range(2):
        value = start_ref[:, 0, p, :]
        low_ref[0, p] = value.astype(BF16).astype(wire)
        moving_ref[0, p] = value
        current_ref[p] = value
    pl.semaphore_wait(barrier, coils - 1 + 2)

    pending = []

    def send(source, target, send_sem, recv_sem, where):
        copy = pltpu.make_async_remote_copy(
            src_ref=source,
            dst_ref=target,
            send_sem=send_sem,
            recv_sem=recv_sem,
            device_id=where,
            device_id_type=MESH,
        )
        pending.append(copy)
        return copy

    paired = frames % 2 == 0
    sibling = frame + 1 - 2 * lax.rem(frame, 2)
    first_core = lax.rem(frame, 2) == 0

    def start(phase, copies):
        if paired and phase in HOLD:
            pl.when(jnp.logical_not(first_core))(lambda: pl.semaphore_wait(turn_sem.at[phase], 1))
        for copy in copies:
            copy.start()

    def sent(phase, copies):
        if paired and phase in HOLD:
            for copy in copies:
                pending[:] = [one for one in pending if one is not copy]

            @pl.when(first_core)
            def _():
                for copy in copies[: HOLD[phase]]:
                    copy.wait_send()
                pl.semaphore_signal(turn_sem.at[phase], inc=1, device_id={"frame": sibling}, device_id_type=MESH)
                for copy in copies[HOLD[phase] :]:
                    copy.wait_send()

            held_back.extend(copies)

    held_back = []

    def spread_image(it, low, full):
        gathers = {
            k: send(low, gather_ref.at[it, k], gather_send.at[it, k], gather_recv.at[it, k], {"coil": peers[k]})
            for k in order
        }
        besides = [
            send(full, beside_ref.at[it, side], beside_send.at[it, side], beside_recv.at[it, side], {"frame": where})
            for side, where in ((0, later), (1, earlier))
        ]
        return gathers, besides

    gathers, besides = spread_image(0, low_ref.at[0], moving_ref.at[0])
    start(0, list(gathers.values()) + besides)

    for place in range(4, 10):
        loads[place].wait()
    loads[10].wait()
    cosine = table_ref[:, :size]
    sine = table_ref[:, size:]
    forward_ref[:size, :size] = cosine
    forward_ref[:size, size:] = -sine
    forward_ref[size:, :size] = sine
    forward_ref[size:, size:] = cosine
    inverse_ref[:size, :size] = cosine
    inverse_ref[:size, size:] = sine
    inverse_ref[size:, :size] = -sine
    inverse_ref[size:, size:] = cosine

    strip = 64
    strips = size // ALIGN
    group = max(d for d in range(1, GROUP + 1) if blocks % d == 0)

    def build(block, carry):
        for first_ref, off_ref, taps_ref, into_ref in (
            (row_first_ref, row_off_ref, row_taps_ref, row_ref),
            (col_first_ref, col_off_ref, col_taps_ref, col_ref),
        ):
            first = first_ref[block] + off_ref[0, block]
            weights = taps_ref[0, block].astype(F32)
            for low in range(0, size, strip):
                distance = lax.broadcasted_iota(jnp.int32, (strip, spoke), 0) + low - first
                matrix = jnp.zeros((strip, spoke), F32)
                for tap in range(taps):
                    matrix = jnp.where(distance == tap, weights[tap : tap + 1], matrix)
                matrix = matrix.astype(BF16)
                if into_ref is col_ref:
                    into_ref[block, low : low + strip, :] = matrix
                else:
                    into_ref[block, low // ALIGN : (low + strip) // ALIGN] = matrix.reshape(-1, ALIGN, spoke)
        row_ref[block, strips] = jnp.zeros((ALIGN, spoke), BF16)
        return carry

    lax.fori_loop(0, blocks, build, 0)
    tally_ref[...] = jnp.zeros_like(tally_ref)
    for p in range(2):
        space_ref[p, strips] = jnp.zeros((ALIGN, size), BF16)
    window = TILE // ALIGN + 1
    deep = window * ALIGN
    for place in range(1, 4):
        loads[place].wait()
    sent(0, list(gathers.values()))
    used = used_ref[0, 0]
    momentum = 1.0

    for it in range(ITERS):
        for k in [0] + order[::-1]:
            if k == 0:
                piece = low_ref[it]
            else:
                gathers[k].wait_recv()
                piece = gather_ref[it, k]
            piece = piece.astype(F32)
            owner = owners[k]
            at = pl.multiple_of(owner * rows, rows)
            at_below = pl.multiple_of(owner * rows + size, rows)
            map_real = maps_ref[0, 0, pl.ds(at, rows), :].astype(F32)
            map_imag = maps_ref[0, 1, pl.ds(at, rows), :].astype(F32)
            real = (map_real * piece[0] - map_imag * piece[1]).astype(BF16).astype(wire)
            imag = (map_real * piece[1] + map_imag * piece[0]).astype(BF16).astype(wire)
            stack_ref[pl.ds(at, rows), :size] = real
            stack_ref[pl.ds(at, rows), size:] = imag
            stack_ref[pl.ds(at_below, rows), :size] = imag
            stack_ref[pl.ds(at_below, rows), size:] = -real
        half = jnp.concatenate(
            [dot(table_ref[...], stack_ref[:, p * size : (p + 1) * size].astype(BF16)).astype(BF16) for p in range(2)],
            axis=1,
        )
        for p in range(2):
            kspace = dot(half, forward_ref[:, p * size : (p + 1) * size]).astype(BF16)
            space_ref[p, :strips] = kspace.reshape(strips, ALIGN, size)
        grid_ref[...] = jnp.zeros_like(grid_ref)

        def predict(turn, total):
            lows = []
            for member in range(group):
                block = turn * group + member
                at = lax.div(row_off_ref[0, block], ALIGN)
                near = jnp.concatenate([space_ref[p, at + i] for p in range(2) for i in range(window)], axis=0)
                across = dot(near, col_ref[block])
                rows_wide = jnp.concatenate([row_ref[block, at + i] for i in range(window)], axis=0).astype(F32)
                measured = samples_ref[0, 0, block].astype(F32)
                active = jnp.where(block < used, 1.0, 0.0)
                for p in range(2):
                    predicted = jnp.sum(
                        across[p * deep : (p + 1) * deep] * rows_wide, axis=0, keepdims=True
                    )
                    resid = (predicted - measured[p : p + 1]) * active
                    total = total + resid * resid
                    lows.append(resid)
            return total, tuple(lows)

        def spread(turn, lows):
            left, sides = ([], []), []
            for member in range(group):
                block = turn * group + member
                sides.append(col_ref[block])
                rows_wide = row_ref[block, :strips].reshape(size, spoke)
                for p in range(2):
                    left[p].append(lows[2 * member + p].astype(BF16) * rows_wide)
            side = jnp.concatenate(sides, axis=1)
            for p in range(2):
                grid_ref[p * size : (p + 1) * size] += dot_nt(jnp.concatenate(left[p], axis=1), side)

        def visit(turn, carry):
            total, lows = carry
            spread(turn - 1, lows)
            return predict(turn, total)

        turns = blocks // group
        carry = predict(0, jnp.zeros((1, spoke), F32))
        total, lows = lax.fori_loop(1, turns, visit, carry) if turns > 1 else carry
        spread(turns - 1, lows)
        tally_ref[it : it + 1, :] = total
        grid_real = grid_ref[:size].astype(BF16)
        grid_imag = grid_ref[size:].astype(BF16)
        turned = jnp.concatenate(
            [
                jnp.concatenate([grid_real, grid_imag], axis=1),
                jnp.concatenate([-grid_imag, grid_real], axis=1),
            ],
            axis=0,
        )
        incomes = {}
        share = size // 2 if halved else size
        for step in range(size // share):
            low = pl.multiple_of((top if step else 1 - top) * share, share) if halved else 0
            span = pl.ds(low, share)
            back_half = dot(table_ref[span, :], turned).astype(BF16)
            coil_back = dot(back_half, inverse_ref[...])
            map_real = maps_ref[0, 0, span, :].astype(F32)
            map_imag = maps_ref[0, 1, span, :].astype(F32)
            back_real = coil_back[:, :size]
            back_imag = coil_back[:, size:]
            grad = (map_real * back_real + map_imag * back_imag, map_real * back_imag - map_imag * back_real)
            for p in range(2):
                outgo_ref[it, p, span, :] = grad[p].astype(wire)
                grad_ref[p, span, :] = grad[p]
            members = order if not halved else [k for k in order if (k < coils // 2) == (step == 1)]
            for k in members:
                at = pl.multiple_of(peers[k] * rows, rows)
                incomes[k] = send(
                    outgo_ref.at[it, :, pl.ds(at, rows), :],
                    income_ref.at[it, k],
                    income_send.at[it, k],
                    income_recv.at[it, k],
                    {"coil": peers[k]},
                )
            if step == 0:
                start(2 * it + 1, [incomes[k] for k in members])
            else:
                for k in members:
                    incomes[k].start()
        tally_copies = []
        if it == ITERS - 1:
            tally_copies = [
                send(tally_ref, tallies_ref.at[k], tally_send.at[k], tally_recv.at[k], {"coil": peers[k]})
                for k in range(1, coils)
            ]
            for copy in tally_copies:
                copy.start()

        for copy in besides:
            copy.wait_recv()
        moving = [moving_ref[it, p] for p in range(2)]
        ahead = [beside_ref[it, 1, p] - moving[p] for p in range(2)]
        behind = [moving[p] - beside_ref[it, 0, p] for p in range(2)]
        floor = smooth_floor * smooth_floor
        ahead_length = jnp.sqrt(ahead[0] * ahead[0] + ahead[1] * ahead[1] + floor)
        behind_length = jnp.sqrt(behind[0] * behind[0] + behind[1] * behind[1] + floor)
        variation = [behind[p] / behind_length - ahead[p] / ahead_length for p in range(2)]

        sent(2 * it + 1, list(incomes.values()))
        here = pl.multiple_of(coil * rows, rows)
        sums = [grad_ref[p, pl.ds(here, rows), :] for p in range(2)]
        for k in range(1, coils):
            incomes[k].wait_recv()
            sums = [sums[p] + income_ref[it, k, p].astype(F32) for p in range(2)]
        descent = [moving[p] - step_size * (sums[p] + tv_weight * variation[p]) for p in range(2)]
        doubled = wavelet_prox(descent, step_size * shrink_weight)
        updated = [doubled[p] * 0.5 for p in range(2)]
        following = (1.0 + math.sqrt(1.0 + 4.0 * momentum * momentum)) / 2.0
        if it == ITERS - 1:
            tiles = size // LANES
            for p in range(2):
                for tile in range(tiles):
                    image_ref[pl.ds(2 * tile + p, rows, stride=2 * tiles), :] = doubled[p][
                        :, tile * LANES : (tile + 1) * LANES
                    ]
        else:
            factor = (momentum - 1.0) / following
            for p in range(2):
                ahead_value = updated[p]
                if factor != 0.0:
                    ahead_value = ahead_value + factor * (updated[p] - current_ref[p])
                low_ref[it + 1, p] = ahead_value.astype(BF16).astype(wire)
                moving_ref[it + 1, p] = ahead_value
                current_ref[p] = updated[p]
            gathers, besides = spread_image(it + 1, low_ref.at[it + 1], moving_ref.at[it + 1])
            start(2 * it + 2, list(gathers.values()) + besides)
            sent(2 * it + 2, list(gathers.values()))
        momentum = following

    tally = tally_ref[...]
    for k in range(1, coils):
        tally_copies[k - 1].wait_recv()
        tally = tally + tallies_ref[k]
    lane = lax.broadcasted_iota(jnp.int32, (1, ITERS), 1)
    misfit = jnp.zeros((1, ITERS), F32)
    for it in range(ITERS):
        misfit = jnp.where(lane == it, jnp.sum(tally[it : it + 1], axis=1, keepdims=True), misfit)
    misfit_ref[...] = misfit
    for copy in pending:
        copy.wait_send()
    if held_back:

        @pl.when(jnp.logical_not(first_core))
        def _():
            for copy in held_back:
                copy.wait_send()


def on_device(coils, frames, table, image, coil_maps, samples, blocks_used, row_off, col_off, row_first, col_first, *taps):
    size = coil_maps.shape[3]
    blocks = samples.shape[2]
    spoke = samples.shape[4]
    rows = size // coils
    wire = BF16 if rows % 16 == 0 else F32
    row_first = jnp.transpose(row_first, (1, 0, 2))
    col_first = jnp.transpose(col_first, (1, 0, 2))
    vmem = pl.BlockSpec(memory_space=pltpu.VMEM)
    operands = (
        image,
        coil_maps,
        samples,
        blocks_used.reshape(1, 1),
        row_off,
        col_off,
        row_first,
        col_first,
        *taps,
        table,
    )
    scalars = (3, 4, 5)
    held = [
        (pltpu.SMEM if place in scalars else pltpu.VMEM)(operand.shape, operand.dtype)
        for place, operand in enumerate(operands)
    ]
    shard = (2, rows, size)
    dma = pltpu.SemaphoreType.DMA
    doubled, misfit = pl.pallas_call(
        functools.partial(kernel, coils, frames),
        out_shape=(
            pltpu.VMEM((2 * rows * size // LANES, LANES), F32),
            pltpu.VMEM((1, ITERS), F32),
        ),
        in_specs=[pl.BlockSpec(memory_space=pl.ANY)] * len(operands),
        out_specs=(vmem, vmem),
        scratch_shapes=held
        + [
            dma((len(operands),)),
            pltpu.VMEM((2 * size, 2 * size), BF16),
            pltpu.VMEM((2 * size, 2 * size), BF16),
            pltpu.VMEM((blocks, size // ALIGN + 1, ALIGN, spoke), BF16),
            pltpu.VMEM((blocks, size, spoke), BF16),
            pltpu.VMEM((2 * size, 2 * size), wire),
            pltpu.VMEM((2, size // ALIGN + 1, ALIGN, size), BF16),
            pltpu.VMEM((2 * size, size), F32),
            pltpu.VMEM((2, size, size), F32),
            pltpu.VMEM((ITERS,) + shard, F32),
            pltpu.VMEM(shard, F32),
            pltpu.VMEM((ITERS,) + shard, wire),
            pltpu.VMEM((ITERS, coils) + shard, wire),
            pltpu.VMEM((ITERS, 2, size, size), wire),
            pltpu.VMEM((ITERS, coils) + shard, wire),
            pltpu.VMEM((ITERS, 2) + shard, F32),
            pltpu.VMEM((8, spoke), F32),
            pltpu.VMEM((coils, 8, spoke), F32),
            dma((ITERS, coils)),
            dma((ITERS, coils)),
            dma((ITERS, coils)),
            dma((ITERS, coils)),
            dma((ITERS, 2)),
            dma((ITERS, 2)),
            dma((coils,)),
            dma((coils,)),
            pltpu.SemaphoreType.REGULAR((2 * ITERS,)),
        ],
        compiler_params=pltpu.CompilerParams(
            collective_id=0, has_side_effects=True, vmem_limit_bytes=56 * 1024 * 1024
        ),
    )(*operands)
    updated = (doubled * 0.5).reshape(rows, size // LANES, 2, LANES).transpose(0, 2, 1, 3)
    scale = 0.5 / (coils * blocks * spoke)
    return updated.reshape(image.shape), jnp.transpose(misfit * scale)


def solution(mesh):
    placed = (
        P("coil", "frame", None, None),
        P("coil", None, None, None),
        P("coil", "frame", None, None, None),
        P("frame"),
        P("frame", None),
        P("frame", None),
        P("frame", None, None),
        P("frame", None, None),
        P("frame", None, None, None),
        P("frame", None, None, None),
    )

    def run(*args):
        table = jnp.asarray(table_pair(args[1].shape[3]))
        body = functools.partial(on_device, mesh.shape["coil"], mesh.shape["frame"], table)
        return jax.shard_map(
            body,
            mesh=mesh,
            in_specs=placed,
            out_specs=(P("coil", "frame", None, None), P(None, "frame")),
            check_vma=False,
        )(*args)

    return run
```

```python
import functools
import math

import jax
import jax.numpy as jnp
import ml_dtypes
import numpy as np
from jax import lax
from jax.experimental import pallas as pl
from jax.experimental.pallas import tpu as pltpu
from jax.sharding import PartitionSpec as P

ITERS = 2
GROUP = 18
TILE = 128
ALIGN = 16
LANES = 128
HOLD = {0: 7, 1: 3, 2: 3}

step_size = 2.0
tv_weight = 0.1
smooth_floor = 0.5
shrink_weight = 0.1

F32 = jnp.float32
BF16 = jnp.bfloat16
MESH = pl.DeviceIdType.MESH


def table_pair(order):
    counter = np.arange(order)
    angle = (counter[:, None] * counter[None, :] % order) * (2.0 * math.pi / order)
    cosine = (np.cos(angle) / math.sqrt(order)).astype(ml_dtypes.bfloat16)
    sine = (np.sin(angle) / math.sqrt(order)).astype(ml_dtypes.bfloat16)
    return np.concatenate([cosine, sine], axis=1)


def partner_of(place, k, count):
    if count & (count - 1):
        return lax.rem(place + k, count)
    result, bit = 0, 1
    while bit < count:
        digit = place // bit % 2
        result = result + (1 - digit if k & bit else digit) * bit
        bit *= 2
    return result


def owner_of(place, k, count):
    if count & (count - 1):
        return lax.rem(place + count - k, count)
    return partner_of(place, k, count)


def dot(left, right):
    return jnp.dot(left, right, preferred_element_type=F32)


def dot_nt(left, right):
    return lax.dot_general(left, right, (((1,), (1,)), ((), ())), preferred_element_type=F32)


def partner(values, axis, parity):
    size = values.shape[axis]
    return jnp.where(
        parity == 0, pltpu.roll(values, size - 1, axis), pltpu.roll(values, 1, axis)
    )


def shrink_pair(real, imag, limit):
    length = jnp.sqrt(real * real + imag * imag)
    factor = jnp.maximum(length - limit, 0.0) / jnp.maximum(length, limit)
    return real * factor, imag * factor


def wavelet_prox(fields, limit):
    shape = fields[0].shape
    row_parity = lax.broadcasted_iota(jnp.int32, shape, 0) % 2
    col_parity = lax.broadcasted_iota(jnp.int32, shape, 1) % 2
    row_sign = jnp.where(row_parity == 0, 1.0, -1.0)
    col_sign = jnp.where(col_parity == 0, 1.0, -1.0)
    parts = []
    for field in fields:
        beside = partner(field, 1, col_parity)
        col_sum = field + beside
        col_diff = (field - beside) * col_sign
        sum_below = partner(col_sum, 0, row_parity)
        diff_below = partner(col_diff, 0, row_parity)
        approx = (col_sum + sum_below) * 0.5
        horiz = (col_diff + diff_below) * 0.5
        vertical = (col_sum - sum_below) * row_sign * 0.5
        diagonal = (col_diff - diff_below) * row_sign * 0.5
        parts.append((approx, horiz, vertical, diagonal))
    real, imag = parts
    horiz = shrink_pair(real[1], imag[1], limit)
    vertical = shrink_pair(real[2], imag[2], limit)
    diagonal = shrink_pair(real[3], imag[3], limit)
    return [
        (parts[p][0] + col_sign * horiz[p] + row_sign * vertical[p] + row_sign * col_sign * diagonal[p])
        for p in range(2)
    ]


def kernel(
    coils,
    frames,
    *refs,
):
    inputs = refs[:11]
    image_ref, misfit_ref = refs[11:13]
    held = refs[13:24]
    input_sem = refs[24]
    loads = []
    for place, (source, target) in enumerate(zip(inputs, held)):
        copy = pltpu.make_async_copy(source, target, input_sem.at[place])
        copy.start()
        loads.append(copy)
    run(coils, frames, loads, *held, image_ref, misfit_ref, *refs[25:])


def run(
    coils,
    frames,
    loads,
    start_ref,
    maps_ref,
    samples_ref,
    used_ref,
    row_off_ref,
    col_off_ref,
    row_first_ref,
    col_first_ref,
    row_taps_ref,
    col_taps_ref,
    table_ref,
    image_ref,
    misfit_ref,
    forward_ref,
    inverse_ref,
    row_ref,
    col_ref,
    stack_ref,
    space_ref,
    grid_ref,
    grad_ref,
    moving_ref,
    current_ref,
    low_ref,
    gather_ref,
    outgo_ref,
    income_ref,
    beside_ref,
    tally_ref,
    tallies_ref,
    gather_send,
    gather_recv,
    income_send,
    income_recv,
    beside_send,
    beside_recv,
    tally_send,
    tally_recv,
    turn_sem,
):
    coil = lax.axis_index("coil")
    frame = lax.axis_index("frame")
    size = maps_ref.shape[2]
    blocks = samples_ref.shape[2]
    spoke = samples_ref.shape[4]
    taps = row_taps_ref.shape[2]
    rows = size // coils
    later = lax.rem(frame + 1, frames)
    earlier = lax.rem(frame + frames - 1, frames)
    peers = [partner_of(coil, k, coils) for k in range(coils)]
    owners = [owner_of(coil, k, coils) for k in range(coils)]
    order = list(range(coils - 1, 0, -1))
    wire = gather_ref.dtype
    halved = coils & (coils - 1) == 0 and coils > 1
    top = coil // max(coils // 2, 1)

    barrier = pltpu.get_barrier_semaphore()
    for k in range(1, coils):
        pl.semaphore_signal(barrier, inc=1, device_id={"coil": peers[k]}, device_id_type=MESH)
    for nearby in (later, earlier):
        pl.semaphore_signal(barrier, inc=1, device_id={"frame": nearby}, device_id_type=MESH)
    loads[0].wait()
    for p in range(2):
        value = start_ref[:, 0, p, :]
        low_ref[0, p] = value.astype(BF16).astype(wire)
        moving_ref[0, p] = value
        current_ref[p] = value
    pl.semaphore_wait(barrier, coils - 1 + 2)

    pending = []

    def send(source, target, send_sem, recv_sem, where):
        copy = pltpu.make_async_remote_copy(
            src_ref=source,
            dst_ref=target,
            send_sem=send_sem,
            recv_sem=recv_sem,
            device_id=where,
            device_id_type=MESH,
        )
        pending.append(copy)
        return copy

    paired = frames % 2 == 0
    sibling = frame + 1 - 2 * lax.rem(frame, 2)
    first_core = lax.rem(frame, 2) == 0

    def start(phase, copies):
        if paired and phase in HOLD:
            pl.when(jnp.logical_not(first_core))(lambda: pl.semaphore_wait(turn_sem.at[phase], 1))
        for copy in copies:
            copy.start()

    def sent(phase, copies):
        if paired and phase in HOLD:
            for copy in copies:
                pending[:] = [one for one in pending if one is not copy]

            @pl.when(first_core)
            def _():
                for copy in copies[: HOLD[phase]]:
                    copy.wait_send()
                pl.semaphore_signal(turn_sem.at[phase], inc=1, device_id={"frame": sibling}, device_id_type=MESH)
                for copy in copies[HOLD[phase] :]:
                    copy.wait_send()

            held_back.extend(copies)

    held_back = []

    def spread_image(it, low, full):
        gathers = {
            k: send(low, gather_ref.at[it, k], gather_send.at[it, k], gather_recv.at[it, k], {"coil": peers[k]})
            for k in order
        }
        besides = [
            send(full, beside_ref.at[it, side], beside_send.at[it, side], beside_recv.at[it, side], {"frame": where})
            for side, where in ((0, later), (1, earlier))
        ]
        return gathers, besides

    gathers, besides = spread_image(0, low_ref.at[0], moving_ref.at[0])
    start(0, list(gathers.values()) + besides)

    for place in range(4, 10):
        loads[place].wait()
    loads[10].wait()
    cosine = table_ref[:, :size]
    sine = table_ref[:, size:]
    forward_ref[:size, :size] = cosine
    forward_ref[:size, size:] = -sine
    forward_ref[size:, :size] = sine
    forward_ref[size:, size:] = cosine
    inverse_ref[:size, :size] = cosine
    inverse_ref[:size, size:] = sine
    inverse_ref[size:, :size] = -sine
    inverse_ref[size:, size:] = cosine

    strip = 64
    strips = size // ALIGN
    group = max(d for d in range(1, GROUP + 1) if blocks % d == 0)

    def build(block, carry):
        for first_ref, off_ref, taps_ref, into_ref in (
            (row_first_ref, row_off_ref, row_taps_ref, row_ref),
            (col_first_ref, col_off_ref, col_taps_ref, col_ref),
        ):
            first = first_ref[block] + off_ref[0, block]
            weights = taps_ref[0, block].astype(F32)
            for low in range(0, size, strip):
                distance = lax.broadcasted_iota(jnp.int32, (strip, spoke), 0) + low - first
                matrix = jnp.zeros((strip, spoke), F32)
                for tap in range(taps):
                    matrix = jnp.where(distance == tap, weights[tap : tap + 1], matrix)
                matrix = matrix.astype(BF16)
                if into_ref is col_ref:
                    into_ref[block, low : low + strip, :] = matrix
                else:
                    into_ref[block, low // ALIGN : (low + strip) // ALIGN] = matrix.reshape(-1, ALIGN, spoke)
        row_ref[block, strips] = jnp.zeros((ALIGN, spoke), BF16)
        return carry

    lax.fori_loop(0, blocks, build, 0)
    tally_ref[...] = jnp.zeros_like(tally_ref)
    for p in range(2):
        space_ref[p, strips] = jnp.zeros((ALIGN, size), BF16)
    window = TILE // ALIGN + 1
    deep = window * ALIGN
    for place in range(1, 4):
        loads[place].wait()
    sent(0, list(gathers.values()))
    used = used_ref[0, 0]
    momentum = 1.0

    for it in range(ITERS):
        for k in [0] + order[::-1]:
            if k == 0:
                piece = low_ref[it]
            else:
                gathers[k].wait_recv()
                piece = gather_ref[it, k]
            piece = piece.astype(F32)
            owner = owners[k]
            at = pl.multiple_of(owner * rows, rows)
            at_below = pl.multiple_of(owner * rows + size, rows)
            map_real = maps_ref[0, 0, pl.ds(at, rows), :].astype(F32)
            map_imag = maps_ref[0, 1, pl.ds(at, rows), :].astype(F32)
            real = (map_real * piece[0] - map_imag * piece[1]).astype(BF16).astype(wire)
            imag = (map_real * piece[1] + map_imag * piece[0]).astype(BF16).astype(wire)
            stack_ref[pl.ds(at, rows), :size] = real
            stack_ref[pl.ds(at, rows), size:] = imag
            stack_ref[pl.ds(at_below, rows), :size] = imag
            stack_ref[pl.ds(at_below, rows), size:] = -real
        half = jnp.concatenate(
            [dot(table_ref[...], stack_ref[:, p * size : (p + 1) * size].astype(BF16)).astype(BF16) for p in range(2)],
            axis=1,
        )
        for p in range(2):
            kspace = dot(half, forward_ref[:, p * size : (p + 1) * size]).astype(BF16)
            space_ref[p, :strips] = kspace.reshape(strips, ALIGN, size)
        grid_ref[...] = jnp.zeros_like(grid_ref)

        def predict(turn, total):
            lows = []
            for member in range(group):
                block = turn * group + member
                at = lax.div(row_off_ref[0, block], ALIGN)
                near = jnp.concatenate([space_ref[p, at + i] for p in range(2) for i in range(window)], axis=0)
                across = dot(near, col_ref[block])
                rows_wide = jnp.concatenate([row_ref[block, at + i] for i in range(window)], axis=0).astype(F32)
                measured = samples_ref[0, 0, block].astype(F32)
                active = jnp.where(block < used, 1.0, 0.0)
                for p in range(2):
                    predicted = jnp.sum(
                        across[p * deep : (p + 1) * deep] * rows_wide, axis=0, keepdims=True
                    )
                    resid = (predicted - measured[p : p + 1]) * active
                    total = total + resid * resid
                    lows.append(resid)
            return total, tuple(lows)

        def spread(turn, lows):
            left, sides = ([], []), []
            for member in range(group):
                block = turn * group + member
                sides.append(col_ref[block])
                rows_wide = row_ref[block, :strips].reshape(size, spoke)
                for p in range(2):
                    left[p].append(lows[2 * member + p].astype(BF16) * rows_wide)
            side = jnp.concatenate(sides, axis=1)
            for p in range(2):
                grid_ref[p * size : (p + 1) * size] += dot_nt(jnp.concatenate(left[p], axis=1), side)

        def visit(turn, carry):
            total, lows = carry
            spread(turn - 1, lows)
            return predict(turn, total)

        turns = blocks // group
        carry = predict(0, jnp.zeros((1, spoke), F32))
        total, lows = lax.fori_loop(1, turns, visit, carry) if turns > 1 else carry
        spread(turns - 1, lows)
        tally_ref[it : it + 1, :] = total
        grid_real = grid_ref[:size].astype(BF16)
        grid_imag = grid_ref[size:].astype(BF16)
        turned = jnp.concatenate(
            [
                jnp.concatenate([grid_real, grid_imag], axis=1),
                jnp.concatenate([-grid_imag, grid_real], axis=1),
            ],
            axis=0,
        )
        incomes = {}
        share = size // 2 if halved else size
        for step in range(size // share):
            low = pl.multiple_of((top if step else 1 - top) * share, share) if halved else 0
            span = pl.ds(low, share)
            back_half = dot(table_ref[span, :], turned).astype(BF16)
            coil_back = dot(back_half, inverse_ref[...])
            map_real = maps_ref[0, 0, span, :].astype(F32)
            map_imag = maps_ref[0, 1, span, :].astype(F32)
            back_real = coil_back[:, :size]
            back_imag = coil_back[:, size:]
            grad = (map_real * back_real + map_imag * back_imag, map_real * back_imag - map_imag * back_real)
            for p in range(2):
                outgo_ref[it, p, span, :] = grad[p].astype(wire)
                grad_ref[p, span, :] = grad[p]
            members = order if not halved else [k for k in order if (k < coils // 2) == (step == 1)]
            for k in members:
                at = pl.multiple_of(peers[k] * rows, rows)
                incomes[k] = send(
                    outgo_ref.at[it, :, pl.ds(at, rows), :],
                    income_ref.at[it, k],
                    income_send.at[it, k],
                    income_recv.at[it, k],
                    {"coil": peers[k]},
                )
            if step == 0:
                start(2 * it + 1, [incomes[k] for k in members])
            else:
                for k in members:
                    incomes[k].start()
        tally_copies = []
        if it == ITERS - 1:
            tally_copies = [
                send(tally_ref, tallies_ref.at[k], tally_send.at[k], tally_recv.at[k], {"coil": peers[k]})
                for k in range(1, coils)
            ]
            for copy in tally_copies:
                copy.start()

        for copy in besides:
            copy.wait_recv()
        moving = [moving_ref[it, p] for p in range(2)]
        ahead = [beside_ref[it, 1, p] - moving[p] for p in range(2)]
        behind = [moving[p] - beside_ref[it, 0, p] for p in range(2)]
        floor = smooth_floor * smooth_floor
        ahead_length = jnp.sqrt(ahead[0] * ahead[0] + ahead[1] * ahead[1] + floor)
        behind_length = jnp.sqrt(behind[0] * behind[0] + behind[1] * behind[1] + floor)
        variation = [behind[p] / behind_length - ahead[p] / ahead_length for p in range(2)]

        sent(2 * it + 1, list(incomes.values()))
        here = pl.multiple_of(coil * rows, rows)
        sums = [grad_ref[p, pl.ds(here, rows), :] for p in range(2)]
        for k in range(1, coils):
            incomes[k].wait_recv()
            sums = [sums[p] + income_ref[it, k, p].astype(F32) for p in range(2)]
        descent = [moving[p] - step_size * (sums[p] + tv_weight * variation[p]) for p in range(2)]
        doubled = wavelet_prox(descent, step_size * shrink_weight)
        updated = [doubled[p] * 0.5 for p in range(2)]
        following = (1.0 + math.sqrt(1.0 + 4.0 * momentum * momentum)) / 2.0
        if it == ITERS - 1:
            tiles = size // LANES
            for p in range(2):
                for tile in range(tiles):
                    image_ref[pl.ds(2 * tile + p, rows, stride=2 * tiles), :] = doubled[p][
                        :, tile * LANES : (tile + 1) * LANES
                    ]
        else:
            factor = (momentum - 1.0) / following
            for p in range(2):
                ahead_value = updated[p]
                if factor != 0.0:
                    ahead_value = ahead_value + factor * (updated[p] - current_ref[p])
                low_ref[it + 1, p] = ahead_value.astype(BF16).astype(wire)
                moving_ref[it + 1, p] = ahead_value
                current_ref[p] = updated[p]
            gathers, besides = spread_image(it + 1, low_ref.at[it + 1], moving_ref.at[it + 1])
            start(2 * it + 2, list(gathers.values()) + besides)
            sent(2 * it + 2, list(gathers.values()))
        momentum = following

    tally = tally_ref[...]
    for k in range(1, coils):
        tally_copies[k - 1].wait_recv()
        tally = tally + tallies_ref[k]
    lane = lax.broadcasted_iota(jnp.int32, (1, ITERS), 1)
    misfit = jnp.zeros((1, ITERS), F32)
    for it in range(ITERS):
        misfit = jnp.where(lane == it, jnp.sum(tally[it : it + 1], axis=1, keepdims=True), misfit)
    misfit_ref[...] = misfit
    for copy in pending:
        copy.wait_send()
    if held_back:

        @pl.when(jnp.logical_not(first_core))
        def _():
            for copy in held_back:
                copy.wait_send()


def on_device(coils, frames, table, image, coil_maps, samples, blocks_used, row_off, col_off, row_first, col_first, *taps):
    size = coil_maps.shape[3]
    blocks = samples.shape[2]
    spoke = samples.shape[4]
    rows = size // coils
    wire = BF16 if rows % 16 == 0 else F32
    row_first = jnp.transpose(row_first, (1, 0, 2))
    col_first = jnp.transpose(col_first, (1, 0, 2))
    vmem = pl.BlockSpec(memory_space=pltpu.VMEM)
    operands = (
        image,
        coil_maps,
        samples,
        blocks_used.reshape(1, 1),
        row_off,
        col_off,
        row_first,
        col_first,
        *taps,
        table,
    )
    scalars = (3, 4, 5)
    held = [
        (pltpu.SMEM if place in scalars else pltpu.VMEM)(operand.shape, operand.dtype)
        for place, operand in enumerate(operands)
    ]
    shard = (2, rows, size)
    dma = pltpu.SemaphoreType.DMA
    doubled, misfit = pl.pallas_call(
        functools.partial(kernel, coils, frames),
        out_shape=(
            pltpu.VMEM((2 * rows * size // LANES, LANES), F32),
            pltpu.VMEM((1, ITERS), F32),
        ),
        in_specs=[pl.BlockSpec(memory_space=pl.ANY)] * len(operands),
        out_specs=(vmem, vmem),
        scratch_shapes=held
        + [
            dma((len(operands),)),
            pltpu.VMEM((2 * size, 2 * size), BF16),
            pltpu.VMEM((2 * size, 2 * size), BF16),
            pltpu.VMEM((blocks, size // ALIGN + 1, ALIGN, spoke), BF16),
            pltpu.VMEM((blocks, size, spoke), BF16),
            pltpu.VMEM((2 * size, 2 * size), wire),
            pltpu.VMEM((2, size // ALIGN + 1, ALIGN, size), BF16),
            pltpu.VMEM((2 * size, size), F32),
            pltpu.VMEM((2, size, size), F32),
            pltpu.VMEM((ITERS,) + shard, F32),
            pltpu.VMEM(shard, F32),
            pltpu.VMEM((ITERS,) + shard, wire),
            pltpu.VMEM((ITERS, coils) + shard, wire),
            pltpu.VMEM((ITERS, 2, size, size), wire),
            pltpu.VMEM((ITERS, coils) + shard, wire),
            pltpu.VMEM((ITERS, 2) + shard, F32),
            pltpu.VMEM((8, spoke), F32),
            pltpu.VMEM((coils, 8, spoke), F32),
            dma((ITERS, coils)),
            dma((ITERS, coils)),
            dma((ITERS, coils)),
            dma((ITERS, coils)),
            dma((ITERS, 2)),
            dma((ITERS, 2)),
            dma((coils,)),
            dma((coils,)),
            pltpu.SemaphoreType.REGULAR((2 * ITERS,)),
        ],
        compiler_params=pltpu.CompilerParams(
            collective_id=0, has_side_effects=True, vmem_limit_bytes=56 * 1024 * 1024
        ),
    )(*operands)

    def finish(doubled_ref, sums_ref, image_ref, misfit_ref):
        image_ref[...] = doubled_ref[...] * 0.5
        misfit_ref[...] = sums_ref[...] * (0.5 / (coils * blocks * spoke))

    doubled, misfit = pl.pallas_call(
        finish,
        out_shape=(jax.ShapeDtypeStruct(doubled.shape, F32), jax.ShapeDtypeStruct(misfit.shape, F32)),
        in_specs=[vmem, vmem],
        out_specs=(vmem, vmem),
    )(pltpu.with_memory_space_constraint(doubled, pltpu.VMEM), pltpu.with_memory_space_constraint(misfit, pltpu.VMEM))
    updated = doubled.reshape(rows, size // LANES, 2, LANES).transpose(0, 2, 1, 3)
    return updated.reshape(image.shape), jnp.transpose(misfit)


def solution(mesh):
    placed = (
        P("coil", "frame", None, None),
        P("coil", None, None, None),
        P("coil", "frame", None, None, None),
        P("frame"),
        P("frame", None),
        P("frame", None),
        P("frame", None, None),
        P("frame", None, None),
        P("frame", None, None, None),
        P("frame", None, None, None),
    )

    def run(*args):
        table = jnp.asarray(table_pair(args[1].shape[3]))
        body = functools.partial(on_device, mesh.shape["coil"], mesh.shape["frame"], table)
        return jax.shard_map(
            body,
            mesh=mesh,
            in_specs=placed,
            out_specs=(P("coil", "frame", None, None), P(None, "frame")),
            check_vma=False,
        )(*args)

    return run
```

```python
import functools
import math

import jax
import jax.numpy as jnp
import ml_dtypes
import numpy as np
from jax import lax
from jax.experimental import pallas as pl
from jax.experimental.pallas import tpu as pltpu
from jax.sharding import PartitionSpec as P

ITERS = 2
GROUP = 18
TILE = 128
ALIGN = 16
LANES = 128
HOLD = {0: 7, 1: 3, 2: 4}

step_size = 2.0
tv_weight = 0.1
smooth_floor = 0.5
shrink_weight = 0.1

F32 = jnp.float32
BF16 = jnp.bfloat16
MESH = pl.DeviceIdType.MESH


def table_pair(order):
    counter = np.arange(order)
    angle = (counter[:, None] * counter[None, :] % order) * (2.0 * math.pi / order)
    cosine = (np.cos(angle) / math.sqrt(order)).astype(ml_dtypes.bfloat16)
    sine = (np.sin(angle) / math.sqrt(order)).astype(ml_dtypes.bfloat16)
    return np.concatenate([cosine, sine], axis=1)


def partner_of(place, k, count):
    if count & (count - 1):
        return lax.rem(place + k, count)
    result, bit = 0, 1
    while bit < count:
        digit = place // bit % 2
        result = result + (1 - digit if k & bit else digit) * bit
        bit *= 2
    return result


def owner_of(place, k, count):
    if count & (count - 1):
        return lax.rem(place + count - k, count)
    return partner_of(place, k, count)


def dot(left, right):
    return jnp.dot(left, right, preferred_element_type=F32)


def dot_nt(left, right):
    return lax.dot_general(left, right, (((1,), (1,)), ((), ())), preferred_element_type=F32)


def partner(values, axis, parity):
    size = values.shape[axis]
    return jnp.where(
        parity == 0, pltpu.roll(values, size - 1, axis), pltpu.roll(values, 1, axis)
    )


def shrink_pair(real, imag, limit):
    length = jnp.sqrt(real * real + imag * imag)
    factor = jnp.maximum(length - limit, 0.0) / jnp.maximum(length, limit)
    return real * factor, imag * factor


def wavelet_prox(fields, limit):
    shape = fields[0].shape
    row_parity = lax.broadcasted_iota(jnp.int32, shape, 0) % 2
    col_parity = lax.broadcasted_iota(jnp.int32, shape, 1) % 2
    row_sign = jnp.where(row_parity == 0, 1.0, -1.0)
    col_sign = jnp.where(col_parity == 0, 1.0, -1.0)
    parts = []
    for field in fields:
        beside = partner(field, 1, col_parity)
        col_sum = field + beside
        col_diff = (field - beside) * col_sign
        sum_below = partner(col_sum, 0, row_parity)
        diff_below = partner(col_diff, 0, row_parity)
        approx = (col_sum + sum_below) * 0.5
        horiz = (col_diff + diff_below) * 0.5
        vertical = (col_sum - sum_below) * row_sign * 0.5
        diagonal = (col_diff - diff_below) * row_sign * 0.5
        parts.append((approx, horiz, vertical, diagonal))
    real, imag = parts
    horiz = shrink_pair(real[1], imag[1], limit)
    vertical = shrink_pair(real[2], imag[2], limit)
    diagonal = shrink_pair(real[3], imag[3], limit)
    return [
        (parts[p][0] + col_sign * horiz[p] + row_sign * vertical[p] + row_sign * col_sign * diagonal[p])
        for p in range(2)
    ]


def kernel(
    coils,
    frames,
    *refs,
):
    inputs = refs[:11]
    image_ref, misfit_ref = refs[11:13]
    held = refs[13:24]
    input_sem = refs[24]
    loads = []
    for place, (source, target) in enumerate(zip(inputs, held)):
        copy = pltpu.make_async_copy(source, target, input_sem.at[place])
        copy.start()
        loads.append(copy)
    run(coils, frames, loads, *held, image_ref, misfit_ref, *refs[25:])


def run(
    coils,
    frames,
    loads,
    start_ref,
    maps_ref,
    samples_ref,
    used_ref,
    row_off_ref,
    col_off_ref,
    row_first_ref,
    col_first_ref,
    row_taps_ref,
    col_taps_ref,
    table_ref,
    image_ref,
    misfit_ref,
    forward_ref,
    inverse_ref,
    row_ref,
    col_ref,
    stack_ref,
    space_ref,
    grid_ref,
    grad_ref,
    moving_ref,
    current_ref,
    low_ref,
    gather_ref,
    outgo_ref,
    income_ref,
    beside_ref,
    tally_ref,
    tallies_ref,
    gather_send,
    gather_recv,
    income_send,
    income_recv,
    beside_send,
    beside_recv,
    tally_send,
    tally_recv,
    turn_sem,
):
    coil = lax.axis_index("coil")
    frame = lax.axis_index("frame")
    size = maps_ref.shape[2]
    blocks = samples_ref.shape[2]
    spoke = samples_ref.shape[4]
    taps = row_taps_ref.shape[2]
    rows = size // coils
    later = lax.rem(frame + 1, frames)
    earlier = lax.rem(frame + frames - 1, frames)
    peers = [partner_of(coil, k, coils) for k in range(coils)]
    owners = [owner_of(coil, k, coils) for k in range(coils)]
    order = list(range(coils - 1, 0, -1))
    wire = gather_ref.dtype
    halved = coils & (coils - 1) == 0 and coils > 1
    top = coil // max(coils // 2, 1)

    barrier = pltpu.get_barrier_semaphore()
    for k in range(1, coils):
        pl.semaphore_signal(barrier, inc=1, device_id={"coil": peers[k]}, device_id_type=MESH)
    for nearby in (later, earlier):
        pl.semaphore_signal(barrier, inc=1, device_id={"frame": nearby}, device_id_type=MESH)
    loads[0].wait()
    for p in range(2):
        value = start_ref[:, 0, p, :]
        low_ref[0, p] = value.astype(BF16).astype(wire)
        moving_ref[0, p] = value
        current_ref[p] = value
    pl.semaphore_wait(barrier, coils - 1 + 2)

    pending = []

    def send(source, target, send_sem, recv_sem, where):
        copy = pltpu.make_async_remote_copy(
            src_ref=source,
            dst_ref=target,
            send_sem=send_sem,
            recv_sem=recv_sem,
            device_id=where,
            device_id_type=MESH,
        )
        pending.append(copy)
        return copy

    paired = frames % 2 == 0
    sibling = frame + 1 - 2 * lax.rem(frame, 2)
    first_core = lax.rem(frame, 2) == 0

    def start(phase, copies):
        if paired and phase in HOLD:
            pl.when(jnp.logical_not(first_core))(lambda: pl.semaphore_wait(turn_sem.at[phase], 1))
        for copy in copies:
            copy.start()

    def sent(phase, copies):
        if paired and phase in HOLD:
            for copy in copies:
                pending[:] = [one for one in pending if one is not copy]

            @pl.when(first_core)
            def _():
                for copy in copies[: HOLD[phase]]:
                    copy.wait_send()
                pl.semaphore_signal(turn_sem.at[phase], inc=1, device_id={"frame": sibling}, device_id_type=MESH)
                for copy in copies[HOLD[phase] :]:
                    copy.wait_send()

            held_back.extend(copies)

    held_back = []

    def spread_image(it, low, full):
        gathers = {
            k: send(low, gather_ref.at[it, k], gather_send.at[it, k], gather_recv.at[it, k], {"coil": peers[k]})
            for k in order
        }
        besides = [
            send(full, beside_ref.at[it, side], beside_send.at[it, side], beside_recv.at[it, side], {"frame": where})
            for side, where in ((0, later), (1, earlier))
        ]
        return gathers, besides

    gathers, besides = spread_image(0, low_ref.at[0], moving_ref.at[0])
    start(0, list(gathers.values()) + besides)

    for place in range(4, 10):
        loads[place].wait()
    loads[10].wait()
    cosine = table_ref[:, :size]
    sine = table_ref[:, size:]
    forward_ref[:size, :size] = cosine
    forward_ref[:size, size:] = -sine
    forward_ref[size:, :size] = sine
    forward_ref[size:, size:] = cosine
    inverse_ref[:size, :size] = cosine
    inverse_ref[:size, size:] = sine
    inverse_ref[size:, :size] = -sine
    inverse_ref[size:, size:] = cosine

    strip = 64
    strips = size // ALIGN
    group = max(d for d in range(1, GROUP + 1) if blocks % d == 0)

    def build(block, carry):
        for first_ref, off_ref, taps_ref, into_ref in (
            (row_first_ref, row_off_ref, row_taps_ref, row_ref),
            (col_first_ref, col_off_ref, col_taps_ref, col_ref),
        ):
            first = first_ref[block] + off_ref[0, block]
            weights = taps_ref[0, block].astype(F32)
            for low in range(0, size, strip):
                distance = lax.broadcasted_iota(jnp.int32, (strip, spoke), 0) + low - first
                matrix = jnp.zeros((strip, spoke), F32)
                for tap in range(taps):
                    matrix = jnp.where(distance == tap, weights[tap : tap + 1], matrix)
                matrix = matrix.astype(BF16)
                if into_ref is col_ref:
                    into_ref[block, low : low + strip, :] = matrix
                else:
                    into_ref[block, low // ALIGN : (low + strip) // ALIGN] = matrix.reshape(-1, ALIGN, spoke)
        row_ref[block, strips] = jnp.zeros((ALIGN, spoke), BF16)
        return carry

    lax.fori_loop(0, blocks, build, 0)
    tally_ref[...] = jnp.zeros_like(tally_ref)
    for p in range(2):
        space_ref[p, strips] = jnp.zeros((ALIGN, size), BF16)
    window = TILE // ALIGN + 1
    deep = window * ALIGN
    for place in range(1, 4):
        loads[place].wait()
    sent(0, list(gathers.values()))
    used = used_ref[0, 0]
    momentum = 1.0

    for it in range(ITERS):
        for k in [0] + order[::-1]:
            if k == 0:
                piece = low_ref[it]
            else:
                gathers[k].wait_recv()
                piece = gather_ref[it, k]
            piece = piece.astype(F32)
            owner = owners[k]
            at = pl.multiple_of(owner * rows, rows)
            at_below = pl.multiple_of(owner * rows + size, rows)
            map_real = maps_ref[0, 0, pl.ds(at, rows), :].astype(F32)
            map_imag = maps_ref[0, 1, pl.ds(at, rows), :].astype(F32)
            real = (map_real * piece[0] - map_imag * piece[1]).astype(BF16).astype(wire)
            imag = (map_real * piece[1] + map_imag * piece[0]).astype(BF16).astype(wire)
            stack_ref[pl.ds(at, rows), :size] = real
            stack_ref[pl.ds(at, rows), size:] = imag
            stack_ref[pl.ds(at_below, rows), :size] = imag
            stack_ref[pl.ds(at_below, rows), size:] = -real
        half = jnp.concatenate(
            [dot(table_ref[...], stack_ref[:, p * size : (p + 1) * size].astype(BF16)).astype(BF16) for p in range(2)],
            axis=1,
        )
        for p in range(2):
            kspace = dot(half, forward_ref[:, p * size : (p + 1) * size]).astype(BF16)
            space_ref[p, :strips] = kspace.reshape(strips, ALIGN, size)
        grid_ref[...] = jnp.zeros_like(grid_ref)

        def predict(turn, total):
            lows = []
            for member in range(group):
                block = turn * group + member
                at = lax.div(row_off_ref[0, block], ALIGN)
                near = jnp.concatenate([space_ref[p, at + i] for p in range(2) for i in range(window)], axis=0)
                across = dot(near, col_ref[block])
                rows_wide = jnp.concatenate([row_ref[block, at + i] for i in range(window)], axis=0).astype(F32)
                measured = samples_ref[0, 0, block].astype(F32)
                active = jnp.where(block < used, 1.0, 0.0)
                for p in range(2):
                    predicted = jnp.sum(
                        across[p * deep : (p + 1) * deep] * rows_wide, axis=0, keepdims=True
                    )
                    resid = (predicted - measured[p : p + 1]) * active
                    total = total + resid * resid
                    lows.append(resid)
            return total, tuple(lows)

        def spread(turn, lows):
            left, sides = ([], []), []
            for member in range(group):
                block = turn * group + member
                sides.append(col_ref[block])
                rows_wide = row_ref[block, :strips].reshape(size, spoke)
                for p in range(2):
                    left[p].append(lows[2 * member + p].astype(BF16) * rows_wide)
            side = jnp.concatenate(sides, axis=1)
            for p in range(2):
                grid_ref[p * size : (p + 1) * size] += dot_nt(jnp.concatenate(left[p], axis=1), side)

        def visit(turn, carry):
            total, lows = carry
            spread(turn - 1, lows)
            return predict(turn, total)

        turns = blocks // group
        carry = predict(0, jnp.zeros((1, spoke), F32))
        total, lows = lax.fori_loop(1, turns, visit, carry) if turns > 1 else carry
        spread(turns - 1, lows)
        tally_ref[it : it + 1, :] = total
        grid_real = grid_ref[:size].astype(BF16)
        grid_imag = grid_ref[size:].astype(BF16)
        turned = jnp.concatenate(
            [
                jnp.concatenate([grid_real, grid_imag], axis=1),
                jnp.concatenate([-grid_imag, grid_real], axis=1),
            ],
            axis=0,
        )
        incomes = {}
        share = size // 2 if halved else size
        for step in range(size // share):
            low = pl.multiple_of((top if step else 1 - top) * share, share) if halved else 0
            span = pl.ds(low, share)
            back_half = dot(table_ref[span, :], turned).astype(BF16)
            coil_back = dot(back_half, inverse_ref[...])
            map_real = maps_ref[0, 0, span, :].astype(F32)
            map_imag = maps_ref[0, 1, span, :].astype(F32)
            back_real = coil_back[:, :size]
            back_imag = coil_back[:, size:]
            grad = (map_real * back_real + map_imag * back_imag, map_real * back_imag - map_imag * back_real)
            for p in range(2):
                outgo_ref[it, p, span, :] = grad[p].astype(wire)
                grad_ref[p, span, :] = grad[p]
            members = order if not halved else [k for k in order if (k < coils // 2) == (step == 1)]
            for k in members:
                at = pl.multiple_of(peers[k] * rows, rows)
                incomes[k] = send(
                    outgo_ref.at[it, :, pl.ds(at, rows), :],
                    income_ref.at[it, k],
                    income_send.at[it, k],
                    income_recv.at[it, k],
                    {"coil": peers[k]},
                )
            if step == 0:
                start(2 * it + 1, [incomes[k] for k in members])
            else:
                for k in members:
                    incomes[k].start()
        tally_copies = []
        if it == ITERS - 1:
            tally_copies = [
                send(tally_ref, tallies_ref.at[k], tally_send.at[k], tally_recv.at[k], {"coil": peers[k]})
                for k in range(1, coils)
            ]
            for copy in tally_copies:
                copy.start()

        for copy in besides:
            copy.wait_recv()
        moving = [moving_ref[it, p] for p in range(2)]
        ahead = [beside_ref[it, 1, p] - moving[p] for p in range(2)]
        behind = [moving[p] - beside_ref[it, 0, p] for p in range(2)]
        floor = smooth_floor * smooth_floor
        ahead_length = jnp.sqrt(ahead[0] * ahead[0] + ahead[1] * ahead[1] + floor)
        behind_length = jnp.sqrt(behind[0] * behind[0] + behind[1] * behind[1] + floor)
        variation = [behind[p] / behind_length - ahead[p] / ahead_length for p in range(2)]

        sent(2 * it + 1, list(incomes.values()))
        here = pl.multiple_of(coil * rows, rows)
        sums = [grad_ref[p, pl.ds(here, rows), :] for p in range(2)]
        for k in range(1, coils):
            incomes[k].wait_recv()
            sums = [sums[p] + income_ref[it, k, p].astype(F32) for p in range(2)]
        descent = [moving[p] - step_size * (sums[p] + tv_weight * variation[p]) for p in range(2)]
        doubled = wavelet_prox(descent, step_size * shrink_weight)
        updated = [doubled[p] * 0.5 for p in range(2)]
        following = (1.0 + math.sqrt(1.0 + 4.0 * momentum * momentum)) / 2.0
        if it == ITERS - 1:
            tiles = size // LANES
            for p in range(2):
                for tile in range(tiles):
                    image_ref[pl.ds(2 * tile + p, rows, stride=2 * tiles), :] = doubled[p][
                        :, tile * LANES : (tile + 1) * LANES
                    ]
        else:
            factor = (momentum - 1.0) / following
            for p in range(2):
                ahead_value = updated[p]
                if factor != 0.0:
                    ahead_value = ahead_value + factor * (updated[p] - current_ref[p])
                low_ref[it + 1, p] = ahead_value.astype(BF16).astype(wire)
                moving_ref[it + 1, p] = ahead_value
                current_ref[p] = updated[p]
            gathers, besides = spread_image(it + 1, low_ref.at[it + 1], moving_ref.at[it + 1])
            start(2 * it + 2, list(gathers.values()) + besides)
            sent(2 * it + 2, list(gathers.values()))
        momentum = following

    tally = tally_ref[...]
    for k in range(1, coils):
        tally_copies[k - 1].wait_recv()
        tally = tally + tallies_ref[k]
    lane = lax.broadcasted_iota(jnp.int32, (1, ITERS), 1)
    misfit = jnp.zeros((1, ITERS), F32)
    for it in range(ITERS):
        misfit = jnp.where(lane == it, jnp.sum(tally[it : it + 1], axis=1, keepdims=True), misfit)
    misfit_ref[...] = misfit
    for copy in pending:
        copy.wait_send()
    if held_back:

        @pl.when(jnp.logical_not(first_core))
        def _():
            for copy in held_back:
                copy.wait_send()


def on_device(coils, frames, table, image, coil_maps, samples, blocks_used, row_off, col_off, row_first, col_first, *taps):
    size = coil_maps.shape[3]
    blocks = samples.shape[2]
    spoke = samples.shape[4]
    rows = size // coils
    wire = BF16 if rows % 16 == 0 else F32
    row_first = jnp.transpose(row_first, (1, 0, 2))
    col_first = jnp.transpose(col_first, (1, 0, 2))
    vmem = pl.BlockSpec(memory_space=pltpu.VMEM)
    operands = (
        image,
        coil_maps,
        samples,
        blocks_used.reshape(1, 1),
        row_off,
        col_off,
        row_first,
        col_first,
        *taps,
        table,
    )
    scalars = (3, 4, 5)
    held = [
        (pltpu.SMEM if place in scalars else pltpu.VMEM)(operand.shape, operand.dtype)
        for place, operand in enumerate(operands)
    ]
    shard = (2, rows, size)
    dma = pltpu.SemaphoreType.DMA
    doubled, misfit = pl.pallas_call(
        functools.partial(kernel, coils, frames),
        out_shape=(
            pltpu.VMEM((2 * rows * size // LANES, LANES), F32),
            pltpu.VMEM((1, ITERS), F32),
        ),
        in_specs=[pl.BlockSpec(memory_space=pl.ANY)] * len(operands),
        out_specs=(vmem, vmem),
        scratch_shapes=held
        + [
            dma((len(operands),)),
            pltpu.VMEM((2 * size, 2 * size), BF16),
            pltpu.VMEM((2 * size, 2 * size), BF16),
            pltpu.VMEM((blocks, size // ALIGN + 1, ALIGN, spoke), BF16),
            pltpu.VMEM((blocks, size, spoke), BF16),
            pltpu.VMEM((2 * size, 2 * size), wire),
            pltpu.VMEM((2, size // ALIGN + 1, ALIGN, size), BF16),
            pltpu.VMEM((2 * size, size), F32),
            pltpu.VMEM((2, size, size), F32),
            pltpu.VMEM((ITERS,) + shard, F32),
            pltpu.VMEM(shard, F32),
            pltpu.VMEM((ITERS,) + shard, wire),
            pltpu.VMEM((ITERS, coils) + shard, wire),
            pltpu.VMEM((ITERS, 2, size, size), wire),
            pltpu.VMEM((ITERS, coils) + shard, wire),
            pltpu.VMEM((ITERS, 2) + shard, F32),
            pltpu.VMEM((8, spoke), F32),
            pltpu.VMEM((coils, 8, spoke), F32),
            dma((ITERS, coils)),
            dma((ITERS, coils)),
            dma((ITERS, coils)),
            dma((ITERS, coils)),
            dma((ITERS, 2)),
            dma((ITERS, 2)),
            dma((coils,)),
            dma((coils,)),
            pltpu.SemaphoreType.REGULAR((2 * ITERS,)),
        ],
        compiler_params=pltpu.CompilerParams(
            collective_id=0, has_side_effects=True, vmem_limit_bytes=56 * 1024 * 1024
        ),
    )(*operands)

    def finish(doubled_ref, sums_ref, image_ref, misfit_ref):
        image_ref[...] = doubled_ref[...] * 0.5
        misfit_ref[...] = sums_ref[...] * (0.5 / (coils * blocks * spoke))

    doubled, misfit = pl.pallas_call(
        finish,
        out_shape=(jax.ShapeDtypeStruct(doubled.shape, F32), jax.ShapeDtypeStruct(misfit.shape, F32)),
        in_specs=[vmem, vmem],
        out_specs=(vmem, vmem),
    )(pltpu.with_memory_space_constraint(doubled, pltpu.VMEM), pltpu.with_memory_space_constraint(misfit, pltpu.VMEM))
    updated = doubled.reshape(rows, size // LANES, 2, LANES).transpose(0, 2, 1, 3)
    return updated.reshape(image.shape), jnp.transpose(misfit)


def solution(mesh):
    placed = (
        P("coil", "frame", None, None),
        P("coil", None, None, None),
        P("coil", "frame", None, None, None),
        P("frame"),
        P("frame", None),
        P("frame", None),
        P("frame", None, None),
        P("frame", None, None),
        P("frame", None, None, None),
        P("frame", None, None, None),
    )

    def run(*args):
        table = jnp.asarray(table_pair(args[1].shape[3]))
        body = functools.partial(on_device, mesh.shape["coil"], mesh.shape["frame"], table)
        return jax.shard_map(
            body,
            mesh=mesh,
            in_specs=placed,
            out_specs=(P("coil", "frame", None, None), P(None, "frame")),
            check_vma=False,
        )(*args)

    return run
```
